128 devices in a mesh: cp: 64 (over x, z, y), hd: 2 (over core).
Axes of the slice: x: 4, y: 4, z: 4, core: 2. Of those that a mesh axis runs over, the one named last changes fastest.
Arguments:
- queries: bfloat16 [12288, 4096], P('cp', 'hd'), may hold values from -48 to 48
- keys: bfloat16 [12288, 1024], P('cp', 'hd'), may hold values from -48 to 48
- values: bfloat16 [12288, 1024], P('cp', 'hd'), may hold values from -6 to 6
- span_table: int32 [128], replicated, may hold values from 0 to 127, as said below
- doc_ids: int32 [12288], replicated, may hold values from 0 to 7, never falling along the last dimension, each value on 1 to 3072 neighbouring positions
- out_weight: bfloat16 [4096, 4096], P('hd'), may hold values from -0.09375 to 0.09375
Outputs:
- mixed: bfloat16 [12288, 4096], P(('cp', 'hd'))
The draws below stay inside these ranges and needn't reach their ends.
Inputs may be any that keep to these rules, and one draw needn't show every extreme that they name: `span_table`: slots 2 j and 2 j + 1 hold two spans c and 127 - c, and every span is held once.
All inputs are finite; a program needn't handle non-finite values.
Results may differ from the reference program's by a relative error of at most 0.0095.
Values may be sent and summed in bfloat16 or wider, within the bound.
A program may use at most 128 MiB of HBM per device.

```python
import math
import jax
import jax.numpy as jnp
import numpy as np
from jax import lax

D = 4096
QUERY_HEADS = 32
KEY_VALUE_HEADS = 8
HEAD_WIDTH = 128
SPAN_TOKENS = 96
DOCS = 8
SPANS = 128
SEQUENCE_TOKENS = 12288


def paired_table(key):
    pairs = jax.random.permutation(jax.random.fold_in(key, 11), SPANS // 2).astype(jnp.int32)
    flips = jax.random.randint(jax.random.fold_in(key, 12), (SPANS // 2,), 0, 2)
    upper = (SPANS - 1 - pairs).astype(jnp.int32)
    first = jnp.where(flips == 1, upper, pairs)
    second = jnp.where(flips == 1, pairs, upper)
    return jnp.stack([first, second], axis=1).reshape(SPANS).astype(jnp.int32)


def draw_span_table(key, part):
    return paired_table(key)


def drawn_pair(key):
    drawn_key_rows = jnp.clip(jax.random.normal(jax.random.fold_in(key, 21), (SEQUENCE_TOKENS, KEY_VALUE_HEADS * HEAD_WIDTH), jnp.float32), -6.0, 6.0)
    base_queries = jnp.clip(jax.random.normal(jax.random.fold_in(key, 22), (SEQUENCE_TOKENS, QUERY_HEADS * HEAD_WIDTH), jnp.float32), -6.0, 6.0)
    new_keys = drawn_key_rows
    new_queries = base_queries
    return (jnp.clip(new_queries, -48.0, 48.0), jnp.clip(new_keys, -48.0, 48.0))


def draw_queries(key, part):
    return drawn_pair(key)[0].astype(jnp.bfloat16)


def draw_keys(key, part):
    return drawn_pair(key)[1].astype(jnp.bfloat16)


def block_levels(rng, dims, shards, smallest, high):
    def one(dim, blocks):
        steps = jax.random.uniform(jax.random.fold_in(jax.random.fold_in(rng, 6), dim), (blocks,), jnp.float32, smallest / len(shards), high / len(shards))
        return jnp.repeat(jnp.exp(steps), dims[dim] // blocks).reshape((-1,) + (1,) * (len(dims) - dim - 1))

    gain = one(*shards[0])
    for cut in shards[1:]:
        gain = gain * one(*cut)
    return gain


def split_up(amount, total, bound, slope):
    portions = [(1 << 20) // math.isqrt(rank ** slope) + 1 for rank in range(2, amount + 1)]
    surplus, given = total - bound - (amount - 1), [1] * (amount - 1)
    while surplus > 0:
        movable = [i for i in range(amount - 1) if given[i] < bound]
        pool, left = sum([portions[i] for i in movable]), surplus
        for i in movable:
            extra = min(bound - given[i], max(1, left * portions[i] // pool), surplus)
            given[i] = given[i] + extra
            surplus = surplus - extra
    return np.array([bound] + given)


def ragged_sizes(own_key, count, total, limit, lean):
    if count == 2:
        one = jax.random.randint(own_key, (), max(1, total - limit), min(limit, total - 1) + 1)
        return jnp.stack([one, total - one])
    sizes = jnp.asarray(split_up(count, total, limit, lean), jnp.int32)
    twos = (count - 1) // 2
    source_of, taker = sizes[1:1 + 2 * twos:2], sizes[2:2 + 2 * twos:2]
    room = jnp.minimum(source_of - 1, limit - taker)
    moved = jax.random.randint(jax.random.fold_in(own_key, 1), (twos,), 0, 1 << 20) % (room + 1)
    sizes = sizes.at[1:1 + 2 * twos:2].set(source_of - moved).at[2:2 + 2 * twos:2].set(taker + moved)
    return sizes[jax.random.permutation(jax.random.fold_in(own_key, 2), count)]


def centred(key, dims, width, bound, cuts=(), kind=jnp.bfloat16):
    gain = block_levels(key, dims, cuts, -0.22, 0.18) if cuts else 1.0
    values = jax.random.normal(key, dims, jnp.float32) * width * gain
    return jnp.minimum(jnp.maximum(values, -bound), bound).astype(kind)


def setup_inputs(seed: int = 0) -> dict:
    seeds = jax.random.split(jax.random.key(seed), 7)
    return {
        "queries": draw_queries(jax.random.fold_in(seeds[6], 71), 0),
        "keys": draw_keys(jax.random.fold_in(seeds[6], 71), 0),
        "values": centred(seeds[2], (SEQUENCE_TOKENS, KEY_VALUE_HEADS * HEAD_WIDTH), 1.0, 6.0, ((0, 64), (1, 2))),
        "span_table": draw_span_table(jax.random.fold_in(seeds[6], 71), 0),
        "doc_ids": jnp.searchsorted(jnp.cumsum(ragged_sizes(seeds[4], DOCS, SEQUENCE_TOKENS, SEQUENCE_TOKENS // 4, 2)), jnp.arange(SEQUENCE_TOKENS), side="right").astype(jnp.int32),
        "out_weight": centred(seeds[5], (QUERY_HEADS * HEAD_WIDTH, D), (QUERY_HEADS * HEAD_WIDTH) ** -0.5, 0.09375, ((0, 2),)),
    }


def reference(queries, keys, values, span_table, doc_ids, out_weight):
    query_group = QUERY_HEADS // KEY_VALUE_HEADS
    scale = HEAD_WIDTH ** -0.5
    rows = jnp.arange(SEQUENCE_TOKENS, dtype=jnp.int32)
    positions = (span_table[rows // SPAN_TOKENS] * SPAN_TOKENS + rows % SPAN_TOKENS).astype(jnp.int32)
    documents = doc_ids[positions]
    key_head_rows = keys.reshape(SEQUENCE_TOKENS, KEY_VALUE_HEADS, HEAD_WIDTH).astype(jnp.float32)
    value_head_rows = values.reshape(SEQUENCE_TOKENS, KEY_VALUE_HEADS, HEAD_WIDTH).astype(jnp.float32)

    def block(index):
        first = (index * SPAN_TOKENS).astype(jnp.int32)
        query_matrix = lax.dynamic_slice_in_dim(queries, first, SPAN_TOKENS, 0)
        query_matrix = query_matrix.reshape(SPAN_TOKENS, KEY_VALUE_HEADS, query_group, HEAD_WIDTH).astype(jnp.float32)
        query_pos = lax.dynamic_slice_in_dim(positions, first, SPAN_TOKENS, 0)
        query_doc = lax.dynamic_slice_in_dim(documents, first, SPAN_TOKENS, 0)
        visible = (positions[None, :] <= query_pos[:, None]) & (documents[None, :] == query_doc[:, None])
        scores = jnp.einsum("qkgd,nkd->kgqn", query_matrix, key_head_rows) * scale
        scores = jnp.where(visible, scores, -1e30)
        best = jnp.max(scores, axis=-1, keepdims=True)
        weights = jnp.where(visible, jnp.exp(scores - best), 0.0)
        denom = jnp.sum(weights, axis=-1)
        rounded = lax.optimization_barrier(weights.astype(jnp.bfloat16)).astype(jnp.float32)
        numer = jnp.einsum("kgqn,nkd->kgqd", rounded, value_head_rows)
        result = numer / denom[..., None]
        return result.transpose(2, 0, 1, 3).reshape(SPAN_TOKENS, QUERY_HEADS * HEAD_WIDTH).astype(jnp.bfloat16)

    attn = lax.map(block, jnp.arange(SEQUENCE_TOKENS // SPAN_TOKENS, dtype=jnp.int32)).reshape(SEQUENCE_TOKENS, QUERY_HEADS * HEAD_WIDTH)
    return jnp.dot(attn, out_weight, preferred_element_type=jnp.float32).astype(jnp.bfloat16)
```

```python
import jax
import jax.numpy as jnp
from jax import lax
from jax.experimental import pallas as pl
from jax.experimental.pallas import tpu as pltpu
from jax.sharding import PartitionSpec as P

HEAD = 128
SPAN = 96
ROWS = 192
GROUP = 512
SLOTS = 64
KEYS = 12288
BLOCK = 384
MESH = pl.DeviceIdType.MESH
NEG = -1e30


def place():
    cp = lax.axis_index("cp")
    core = lax.axis_index("hd")
    x = cp // 16
    z = (cp // 4) % 4
    y = cp % 4
    band = z // 2
    cross = (band - core) * (band - core)
    return cp, core, x, z, y, band, cross


def chip(x, z, y):
    return x * 16 + z * 4 + y


def enter_group(x, z, y, core, others):
    barrier = pltpu.get_barrier_semaphore()
    count = 0
    for dz in range(2):
        zz = z if dz == 0 else 3 - z
        for dy in range(4):
            for dc in range(2):
                if dz + dy + dc == 0:
                    continue
                target = (chip(x, zz, (y + dy) % 4), (core + dc) % 2)
                pl.semaphore_signal(barrier, inc=1, device_id=target, device_id_type=MESH)
                count += 1
    for target in others:
        pl.semaphore_signal(barrier, inc=1, device_id=target, device_id_type=MESH)
        count += 1
    pl.semaphore_wait(barrier, count)


def spread_kernel(
    q_ref, k_ref, v_ref, qr_ref, kv_ref, ex_send, ex_recv, q_send, q_recv, ag_send, ag_recv, dd_send, dd_recv
):
    cp, core, x, z, y, band, cross = place()
    zo = 3 - z
    za = z + 1 - 2 * (z % 2)
    zao = 3 - za
    xr, xl, xo = (x + 1) % 4, (x + 3) % 4, (x + 2) % 4
    right = (chip(xr, z, y), core)
    left = (chip(xl, z, y), core)
    across = (chip(x, za, y), core)
    twin = (cp, 1 - core)
    enter_group(x, z, y, core, (right, left, across))

    zt = z + cross * (3 - 2 * z)
    finish = []

    def push(src, dst, device, send_sem, recv_sem, own):
        copy = pltpu.make_async_remote_copy(
            src_ref=src, dst_ref=dst, send_sem=send_sem, recv_sem=recv_sem, device_id=device, device_id_type=MESH
        )
        if own is None:
            copy.start()
            finish.append((None, copy))
            return

        @pl.when(own)
        def _():
            pltpu.make_async_copy(src, dst, recv_sem).start()

        @pl.when(jnp.logical_not(own))
        def _():
            copy.start()

        finish.append((own, copy))

    for dy in range(4):
        yy = (y + dy) % 4
        home = chip(x, zt, yy)
        cols = pl.ds(pl.multiple_of(yy * HEAD, HEAD), HEAD)
        for t, ref in enumerate((k_ref, v_ref)):
            own = (cross + jnp.abs(core - t) == 0) if dy == 0 else None
            push(
                ref.at[:, cols],
                kv_ref.at[t, cp],
                (home, t),
                ex_send.at[dy * 2 + t],
                ex_recv.at[cross],
                own,
            )
    keeper = core + cross * (1 - 2 * core)
    for dy in range(4):
        yy = (y + dy) % 4
        cols = pl.ds(pl.multiple_of(yy * GROUP, GROUP), GROUP)
        own = (cross == 0) if dy == 0 else None
        push(
            q_ref.at[:, cols],
            qr_ref.at[y],
            (chip(x, zt, yy), keeper),
            q_send.at[dy],
            q_recv,
            own,
        )

    def part(t, xs, zs):
        return kv_ref.at[t, pl.ds(xs * 16 + zs * 4, 4)]

    def arrive(t, xs, zs, sem):
        ref = part(t, xs, zs)
        pltpu.make_async_copy(ref, ref, sem).wait()

    def run(t, steps):
        sends = []
        for kind, xs, zs, targets in steps:
            if kind == "own":
                arrive(t, xs, zs, ex_recv.at[0])
            elif kind == "pair":
                arrive(t, xs, zs, ex_recv.at[1])
            else:
                arrive(t, xs, zs, ag_recv.at[xs * 4 + zs])
            for device in targets:
                copy = pltpu.make_async_remote_copy(
                    src_ref=part(t, xs, zs),
                    dst_ref=part(t, xs, zs),
                    send_sem=ag_send.at[len(sends)],
                    recv_sem=ag_recv.at[xs * 4 + zs],
                    device_id=device,
                    device_id_type=MESH,
                )
                copy.start()
                sends.append(copy)
            copy = pltpu.make_async_remote_copy(
                src_ref=part(t, xs, zs),
                dst_ref=part(t, xs, zs),
                send_sem=dd_send.at[xs * 4 + zs],
                recv_sem=dd_recv.at[xs * 4 + zs],
                device_id=twin,
                device_id_type=MESH,
            )
            copy.start()
        for copy in sends:
            copy.wait_send()

    @pl.when(core == 0)
    def _():
        run(
            0,
            (
                ("own", x, z, (across, right, left)),
                ("pair", x, zo, (across, left, right)),
                ("got", x, za, (right, left)),
                ("got", x, zao, (left, right)),
                ("got", xl, z, (right,)),
                ("got", xr, z, ()),
                ("got", xr, zo, (left,)),
                ("got", xl, zo, ()),
                ("got", xl, za, (right,)),
                ("got", xr, za, ()),
                ("got", xr, zao, (left,)),
                ("got", xl, zao, ()),
                ("got", xo, z, ()),
                ("got", xo, zo, ()),
                ("got", xo, za, ()),
                ("got", xo, zao, ()),
            ),
        )

    @pl.when(core == 1)
    def _():
        run(
            1,
            (
                ("own", x, z, (right, left, across)),
                ("pair", x, zo, (left, right, across)),
                ("got", xl, z, (right, across)),
                ("got", xr, z, (across,)),
                ("got", xr, zo, (left, across)),
                ("got", xl, zo, (across,)),
                ("got", x, za, ()),
                ("got", x, zao, ()),
                ("got", xo, z, (across,)),
                ("got", xo, zo, (across,)),
                ("got", xl, za, ()),
                ("got", xr, za, ()),
                ("got", xr, zao, ()),
                ("got", xl, zao, ()),
                ("got", xo, za, ()),
                ("got", xo, zao, ()),
            ),
        )

    for piece in range(16):
        ref = kv_ref.at[1 - core, pl.ds(piece * 4, 4)]
        pltpu.make_async_copy(ref, ref, dd_recv.at[piece]).wait()
        ref = kv_ref.at[core, pl.ds(piece * 4, 4)]
        pltpu.make_async_copy(ref, ref, dd_send.at[piece]).wait()
    pltpu.make_async_copy(qr_ref, qr_ref, q_recv).wait()
    for own, copy in finish:
        if own is None:
            copy.wait_send()
        else:

            @pl.when(jnp.logical_not(own))
            def _():
                copy.wait_send()


def spread(queries, keys, values):
    return pl.pallas_call(
        spread_kernel,
        out_shape=(
            jax.ShapeDtypeStruct((4, ROWS, GROUP), jnp.bfloat16),
            jax.ShapeDtypeStruct((2, SLOTS, ROWS, HEAD), jnp.bfloat16),
        ),
        in_specs=[pl.BlockSpec(memory_space=pl.ANY)] * 3,
        out_specs=[pl.BlockSpec(memory_space=pl.ANY)] * 2,
        scratch_shapes=[
            pltpu.SemaphoreType.DMA((8,)),
            pltpu.SemaphoreType.DMA((2,)),
            pltpu.SemaphoreType.DMA((4,)),
            pltpu.SemaphoreType.DMA,
            pltpu.SemaphoreType.DMA((14,)),
            pltpu.SemaphoreType.DMA((16,)),
            pltpu.SemaphoreType.DMA((16,)),
            pltpu.SemaphoreType.DMA((16,)),
        ],
        compiler_params=pltpu.CompilerParams(collective_id=0, has_side_effects=True),
        name="spread",
    )(queries, keys, values)


def attend_kernel(span_ref, doc_ref, q_ref, kv_hbm, o_ref, kv_ref, sem):
    cp, core, x, z, y, band, cross = place()
    zs = z + cross * (3 - 2 * z)

    def fetch(slot, carry):
        span = span_ref[slot]
        pltpu.make_async_copy(
            kv_hbm.at[:, slot // 2, pl.ds(pl.multiple_of((slot % 2) * SPAN, SPAN), SPAN), :],
            kv_ref.at[:, pl.ds(pl.multiple_of(BLOCK + span * SPAN, SPAN), SPAN), :],
            sem,
        ).start()
        return carry

    lax.fori_loop(0, 2 * SLOTS, fetch, 0)
    kv_ref[:, 0:BLOCK, :] = jnp.zeros((2, BLOCK, HEAD), jnp.bfloat16)
    docs = doc_ref[...]
    starts = [jnp.sum((docs < d).astype(jnp.float32)).astype(jnp.int32) for d in range(1, 8)]
    whole = kv_ref.at[:, pl.ds(BLOCK, KEYS), :]
    pltpu.make_async_copy(whole, whole, sem).wait()
    factor = HEAD ** (-0.5) * 1.4426950408889634

    def query(index, carry):
        src = index // 2
        rows = pl.ds(pl.multiple_of((index % 2) * SPAN, SPAN), SPAN)
        span = span_ref[2 * chip(x, zs, src) + index % 2]
        first = span * SPAN
        q = q_ref[src, rows, :]
        q = jnp.concatenate([q[:, h * HEAD : (h + 1) * HEAD] for h in range(4)], axis=0)
        hi = first + lax.broadcasted_iota(jnp.int32, (SPAN, 1), 0)
        lo = jnp.zeros((SPAN, 1), jnp.int32)
        lowest = jnp.int32(0)
        for start in starts:
            lo = jnp.where(hi >= start, start, lo)
            lowest = jnp.where(first >= start, start, lowest)
        hi = jnp.concatenate([hi] * 4, axis=0)
        lo = jnp.concatenate([lo] * 4, axis=0)
        blocks = (first + SPAN - lowest + BLOCK - 1) // BLOCK

        def visit(step, state):
            best, total, accum = state
            base = first + SPAN - BLOCK * (step + 1)
            at = pl.ds(pl.multiple_of(BLOCK + base, SPAN), BLOCK)
            k = kv_ref[0, at, :]
            v = kv_ref[1, at, :]
            s = lax.dot_general(q, k, (((1,), (1,)), ((), ())), preferred_element_type=jnp.float32)
            pos = base + lax.broadcasted_iota(jnp.int32, (4 * SPAN, BLOCK), 1)
            s = jnp.where((pos >= lo) & (pos <= hi), s, NEG)
            new = jnp.maximum(best, jnp.max(s, axis=1, keepdims=True))
            w = jnp.exp2((s - new) * factor)
            fade = jnp.exp2((best - new) * factor)
            total = total * fade + jnp.sum(w, axis=1, keepdims=True)
            accum = accum * fade + jnp.dot(w.astype(jnp.bfloat16), v, preferred_element_type=jnp.float32)
            return new, total, accum

        best, total, accum = lax.fori_loop(
            0,
            blocks,
            visit,
            (
                jnp.full((4 * SPAN, 1), NEG, jnp.float32),
                jnp.zeros((4 * SPAN, 1), jnp.float32),
                jnp.zeros((4 * SPAN, HEAD), jnp.float32),
            ),
        )
        out = (accum / total).astype(jnp.bfloat16)
        for h in range(4):
            o_ref[src, rows, h * HEAD : (h + 1) * HEAD] = out[h * SPAN : (h + 1) * SPAN]
        return carry

    lax.fori_loop(0, 8, query, 0)


def attend(span_table, doc_ids, q, kv):
    return pl.pallas_call(
        attend_kernel,
        out_shape=jax.ShapeDtypeStruct((4, ROWS, GROUP), jnp.bfloat16),
        in_specs=[
            pl.BlockSpec(memory_space=pltpu.SMEM),
            pl.BlockSpec(memory_space=pltpu.VMEM),
            pl.BlockSpec(memory_space=pltpu.VMEM),
            pl.BlockSpec(memory_space=pl.ANY),
        ],
        out_specs=pl.BlockSpec(memory_space=pltpu.VMEM),
        scratch_shapes=[
            pltpu.VMEM((2, BLOCK + KEYS, HEAD), jnp.bfloat16),
            pltpu.SemaphoreType.DMA,
        ],
        compiler_params=pltpu.CompilerParams(vmem_limit_bytes=40 * 1024 * 1024),
        name="attend",
    )(span_table, doc_ids.reshape(KEYS // 128, 128), q, kv)


CHUNK = 512
CHUNKS = 8


def project_kernel(
    o_ref, w_ref, out_ref, attn, weight, share, theirs, w_sem, b_send, b_recv, s_send, s_recv
):
    cp, core, x, z, y, band, cross = place()
    for n in range(CHUNKS):
        pltpu.make_async_copy(w_ref.at[:, pl.ds(n * CHUNK, CHUNK)], weight.at[n], w_sem.at[n]).start()
    enter_group(x, z, y, core, ())
    zs = z + cross * (3 - 2 * z)
    copies = []
    for dy in range(4):
        yy = (y + dy) % 4
        src, dst = o_ref.at[yy], attn.at[y]
        copy = pltpu.make_async_remote_copy(
            src_ref=src,
            dst_ref=dst,
            send_sem=b_send.at[dy],
            recv_sem=b_recv,
            device_id=(chip(x, zs, yy), band),
            device_id_type=MESH,
        )
        copies.append(copy)
        if dy == 0:

            @pl.when(cross == 0)
            def _():
                pltpu.make_async_copy(src, dst, b_recv).start()

            @pl.when(cross != 0)
            def _():
                copy.start()
        else:
            copy.start()
    pltpu.make_async_copy(attn, attn, b_recv).wait()
    mine = pl.ds(pl.multiple_of(core * SPAN, SPAN), SPAN)
    yours = pl.ds(pl.multiple_of((1 - core) * SPAN, SPAN), SPAN)

    def give(n):
        return pltpu.make_async_remote_copy(
            src_ref=share.at[n, yours],
            dst_ref=theirs.at[n],
            send_sem=s_send.at[n],
            recv_sem=s_recv.at[n],
            device_id=(cp, 1 - core),
            device_id_type=MESH,
        )

    def multiply(n, carry):
        pltpu.make_async_copy(weight.at[n], weight.at[n], w_sem.at[n]).wait()
        acc = jnp.dot(attn[0], weight[n, 0:GROUP, :], preferred_element_type=jnp.float32)
        for k in range(1, 4):
            acc += jnp.dot(attn[k], weight[n, k * GROUP : (k + 1) * GROUP, :], preferred_element_type=jnp.float32)
        share[n] = acc.astype(jnp.bfloat16)
        give(n).start()
        return carry

    lax.fori_loop(0, CHUNKS, multiply, 0)

    def add(n, carry):
        give(n).wait()
        cols = pl.ds(pl.multiple_of(n * CHUNK, CHUNK), CHUNK)
        total = share[n, mine, :].astype(jnp.float32) + theirs[n].astype(jnp.float32)
        out_ref[:, cols] = total.astype(jnp.bfloat16)
        return carry

    lax.fori_loop(0, CHUNKS, add, 0)
    for dy, copy in enumerate(copies):
        if dy == 0:

            @pl.when(cross != 0)
            def _():
                copy.wait_send()
        else:
            copy.wait_send()


def project(o, weight):
    return pl.pallas_call(
        project_kernel,
        out_shape=jax.ShapeDtypeStruct((SPAN, 4096), jnp.bfloat16),
        in_specs=[pl.BlockSpec(memory_space=pl.ANY)] * 2,
        out_specs=pl.BlockSpec(memory_space=pltpu.VMEM),
        scratch_shapes=[
            pltpu.VMEM((4, ROWS, GROUP), jnp.bfloat16),
            pltpu.VMEM((CHUNKS, 2048, CHUNK), jnp.bfloat16),
            pltpu.VMEM((CHUNKS, ROWS, CHUNK), jnp.bfloat16),
            pltpu.VMEM((CHUNKS, SPAN, CHUNK), jnp.bfloat16),
            pltpu.SemaphoreType.DMA((CHUNKS,)),
            pltpu.SemaphoreType.DMA((4,)),
            pltpu.SemaphoreType.DMA,
            pltpu.SemaphoreType.DMA((CHUNKS,)),
            pltpu.SemaphoreType.DMA((CHUNKS,)),
        ],
        compiler_params=pltpu.CompilerParams(
            collective_id=1, has_side_effects=True, vmem_limit_bytes=40 * 1024 * 1024
        ),
        name="project",
    )(o, weight)


def local(queries, keys, values, span_table, doc_ids, out_weight):
    q, kv = spread(queries, keys, values)
    o = attend(span_table, doc_ids, q, kv)
    return project(o, out_weight)


def solution(mesh):
    return jax.shard_map(
        local,
        mesh=mesh,
        in_specs=(P("cp", "hd"), P("cp", "hd"), P("cp", "hd"), P(), P(), P("hd", None)),
        out_specs=P(("cp", "hd"), None),
        check_vma=False,
    )
```

```python
import jax
import jax.numpy as jnp
from jax import lax
from jax.experimental import pallas as pl
from jax.experimental.pallas import tpu as pltpu
from jax.sharding import PartitionSpec as P

HEAD = 128
SPAN = 96
ROWS = 192
GROUP = 512
SLOTS = 64
KEYS = 12288
BLOCK = 384
MESH = pl.DeviceIdType.MESH
NEG = -1e30


def place():
    cp = lax.axis_index("cp")
    core = lax.axis_index("hd")
    x = cp // 16
    z = (cp // 4) % 4
    y = cp % 4
    band = z // 2
    cross = (band - core) * (band - core)
    return cp, core, x, z, y, band, cross


def chip(x, z, y):
    return x * 16 + z * 4 + y


def enter_group(x, z, y, core, others):
    barrier = pltpu.get_barrier_semaphore()
    count = 0
    for dz in range(2):
        zz = z if dz == 0 else 3 - z
        for dy in range(4):
            for dc in range(2):
                if dz + dy + dc == 0:
                    continue
                target = (chip(x, zz, (y + dy) % 4), (core + dc) % 2)
                pl.semaphore_signal(barrier, inc=1, device_id=target, device_id_type=MESH)
                count += 1
    for target in others:
        pl.semaphore_signal(barrier, inc=1, device_id=target, device_id_type=MESH)
        count += 1
    pl.semaphore_wait(barrier, count)


def spread_kernel(
    q_ref, k_ref, v_ref, qr_ref, kv_ref, ex_send, ex_recv, q_send, q_recv, ag_send, ag_recv, dd_send, dd_recv
):
    cp, core, x, z, y, band, cross = place()
    zo = 3 - z
    za = z + 1 - 2 * (z % 2)
    zao = 3 - za
    xr, xl, xo = (x + 1) % 4, (x + 3) % 4, (x + 2) % 4
    right = (chip(xr, z, y), core)
    left = (chip(xl, z, y), core)
    across = (chip(x, za, y), core)
    twin = (cp, 1 - core)
    enter_group(x, z, y, core, (right, left, across))

    zt = z + cross * (3 - 2 * z)
    finish = []

    def push(src, dst, device, send_sem, recv_sem, own):
        copy = pltpu.make_async_remote_copy(
            src_ref=src, dst_ref=dst, send_sem=send_sem, recv_sem=recv_sem, device_id=device, device_id_type=MESH
        )
        if own is None:
            copy.start()
            finish.append((None, copy))
            return

        @pl.when(own)
        def _():
            pltpu.make_async_copy(src, dst, recv_sem).start()

        @pl.when(jnp.logical_not(own))
        def _():
            copy.start()

        finish.append((own, copy))

    for dy in range(4):
        yy = (y + dy) % 4
        home = chip(x, zt, yy)
        cols = pl.ds(pl.multiple_of(yy * HEAD, HEAD), HEAD)
        for t, ref in enumerate((k_ref, v_ref)):
            own = (cross + jnp.abs(core - t) == 0) if dy == 0 else None
            push(
                ref.at[:, cols],
                kv_ref.at[t, cp],
                (home, t),
                ex_send.at[dy * 2 + t],
                ex_recv.at[cross],
                own,
            )
    keeper = core + cross * (1 - 2 * core)
    for dy in range(4):
        yy = (y + dy) % 4
        cols = pl.ds(pl.multiple_of(yy * GROUP, GROUP), GROUP)
        own = (cross == 0) if dy == 0 else None
        push(
            q_ref.at[:, cols],
            qr_ref.at[y],
            (chip(x, zt, yy), keeper),
            q_send.at[dy],
            q_recv,
            own,
        )

    def part(t, xs, zs):
        return kv_ref.at[t, pl.ds(xs * 16 + zs * 4, 4)]

    def arrive(t, xs, zs, sem):
        ref = part(t, xs, zs)
        pltpu.make_async_copy(ref, ref, sem).wait()

    def run(t, steps):
        sends = []
        for kind, xs, zs, targets in steps:
            if kind == "own":
                arrive(t, xs, zs, ex_recv.at[0])
            elif kind == "pair":
                arrive(t, xs, zs, ex_recv.at[1])
            else:
                arrive(t, xs, zs, ag_recv.at[xs * 4 + zs])
            for device in targets:
                copy = pltpu.make_async_remote_copy(
                    src_ref=part(t, xs, zs),
                    dst_ref=part(t, xs, zs),
                    send_sem=ag_send.at[len(sends)],
                    recv_sem=ag_recv.at[xs * 4 + zs],
                    device_id=device,
                    device_id_type=MESH,
                )
                copy.start()
                sends.append(copy)
            copy = pltpu.make_async_remote_copy(
                src_ref=part(t, xs, zs),
                dst_ref=part(t, xs, zs),
                send_sem=dd_send.at[xs * 4 + zs],
                recv_sem=dd_recv.at[xs * 4 + zs],
                device_id=twin,
                device_id_type=MESH,
            )
            copy.start()
        for copy in sends:
            copy.wait_send()

    @pl.when(core == 0)
    def _():
        run(
            0,
            (
                ("own", x, z, (across, right, left)),
                ("pair", x, zo, (across, left, right)),
                ("got", x, za, (right, left)),
                ("got", x, zao, (left, right)),
                ("got", xl, z, (right,)),
                ("got", xr, z, ()),
                ("got", xr, zo, (left,)),
                ("got", xl, zo, ()),
                ("got", xl, za, (right,)),
                ("got", xr, za, ()),
                ("got", xr, zao, (left,)),
                ("got", xl, zao, ()),
                ("got", xo, z, ()),
                ("got", xo, zo, ()),
                ("got", xo, za, ()),
                ("got", xo, zao, ()),
            ),
        )

    @pl.when(core == 1)
    def _():
        run(
            1,
            (
                ("own", x, z, (right, left, across)),
                ("pair", x, zo, (left, right, across)),
                ("got", xl, z, (right, across)),
                ("got", xr, z, (across,)),
                ("got", xr, zo, (left, across)),
                ("got", xl, zo, (across,)),
                ("got", x, za, ()),
                ("got", x, zao, ()),
                ("got", xo, z, (across,)),
                ("got", xo, zo, (across,)),
                ("got", xl, za, ()),
                ("got", xr, za, ()),
                ("got", xr, zao, ()),
                ("got", xl, zao, ()),
                ("got", xo, za, ()),
                ("got", xo, zao, ()),
            ),
        )

    for piece in range(16):
        ref = kv_ref.at[1 - core, pl.ds(piece * 4, 4)]
        pltpu.make_async_copy(ref, ref, dd_recv.at[piece]).wait()
        ref = kv_ref.at[core, pl.ds(piece * 4, 4)]
        pltpu.make_async_copy(ref, ref, dd_send.at[piece]).wait()
    pltpu.make_async_copy(qr_ref, qr_ref, q_recv).wait()
    for own, copy in finish:
        if own is None:
            copy.wait_send()
        else:

            @pl.when(jnp.logical_not(own))
            def _():
                copy.wait_send()


def spread(queries, keys, values):
    return pl.pallas_call(
        spread_kernel,
        out_shape=(
            jax.ShapeDtypeStruct((4, ROWS, GROUP), jnp.bfloat16),
            jax.ShapeDtypeStruct((2, SLOTS, ROWS, HEAD), jnp.bfloat16),
        ),
        in_specs=[pl.BlockSpec(memory_space=pltpu.HBM)] * 3,
        out_specs=[pl.BlockSpec(memory_space=pltpu.VMEM)] * 2,
        scratch_shapes=[
            pltpu.SemaphoreType.DMA((8,)),
            pltpu.SemaphoreType.DMA((2,)),
            pltpu.SemaphoreType.DMA((4,)),
            pltpu.SemaphoreType.DMA,
            pltpu.SemaphoreType.DMA((14,)),
            pltpu.SemaphoreType.DMA((16,)),
            pltpu.SemaphoreType.DMA((16,)),
            pltpu.SemaphoreType.DMA((16,)),
        ],
        compiler_params=pltpu.CompilerParams(
            collective_id=0, has_side_effects=True, vmem_limit_bytes=16 * 1024 * 1024
        ),
        cost_estimate=pl.CostEstimate(flops=20_000_000_000, bytes_accessed=40_000_000, transcendentals=0),
        name="spread",
    )(queries, keys, values)


def attend_kernel(span_ref, doc_ref, q_ref, kv_ref, o_ref, slot_ref):
    cp, core, x, z, y, band, cross = place()
    zs = z + cross * (3 - 2 * z)

    def invert(slot, carry):
        slot_ref[span_ref[slot]] = slot
        return carry

    lax.fori_loop(0, 2 * SLOTS, invert, 0, unroll=8)
    docs = doc_ref[...]
    starts = [jnp.sum((docs < d).astype(jnp.float32)).astype(jnp.int32) for d in range(1, 8)]
    factor = HEAD ** (-0.5) * 1.4426950408889634
    width = 4 * SPAN

    def query(index, carry):
        src = index // 2
        rows = pl.ds(pl.multiple_of((index % 2) * SPAN, SPAN), SPAN)
        span = span_ref[2 * chip(x, zs, src) + index % 2]
        first = span * SPAN
        q = q_ref[src, rows, :]
        q = jnp.concatenate([q[:, h * HEAD : (h + 1) * HEAD] for h in range(4)], axis=0)
        hi = first + lax.broadcasted_iota(jnp.int32, (1, width), 1) % SPAN
        lo = jnp.zeros((1, width), jnp.int32)
        lowest = jnp.int32(0)
        for start in starts:
            lo = jnp.where(hi >= start, start, lo)
            lowest = jnp.where(first >= start, start, lowest)
        blocks = (first + SPAN - lowest + BLOCK - 1) // BLOCK

        def visit(step, state):
            best, total, accum = state
            low = span - 3 - 4 * step
            slots = [slot_ref[jnp.maximum(low + j, 0)] for j in range(4)]
            k = jnp.concatenate([kv_ref[0, slot] for slot in slots], axis=0)
            v = jnp.concatenate([kv_ref[1, slot] for slot in slots], axis=0)
            s = lax.dot_general(k, q, (((1,), (1,)), ((), ())), preferred_element_type=jnp.float32)
            pos = lax.broadcasted_iota(jnp.int32, (BLOCK, width), 0)
            base = low * SPAN
            s = jnp.where((pos >= lo - base) & (pos <= hi - base), s, NEG)
            new = jnp.maximum(best, jnp.max(s, axis=0, keepdims=True))
            w = jnp.exp2((s - new) * factor)
            fade = jnp.exp2((best - new) * factor)
            total = total * fade + jnp.sum(w, axis=0, keepdims=True)
            accum = accum * fade + lax.dot_general(
                v, w.astype(jnp.bfloat16), (((0,), (0,)), ((), ())), preferred_element_type=jnp.float32
            )
            return new, total, accum

        best, total, accum = lax.fori_loop(
            0,
            blocks,
            visit,
            (
                jnp.full((1, width), NEG, jnp.float32),
                jnp.zeros((1, width), jnp.float32),
                jnp.zeros((HEAD, width), jnp.float32),
            ),
        )
        out = (accum / total).T.astype(jnp.bfloat16)
        for h in range(4):
            o_ref[src, rows, h * HEAD : (h + 1) * HEAD] = out[h * SPAN : (h + 1) * SPAN]
        return carry

    lax.fori_loop(0, 8, query, 0)


def attend(span_table, doc_ids, q, kv):
    return pl.pallas_call(
        attend_kernel,
        out_shape=jax.ShapeDtypeStruct((4, ROWS, GROUP), jnp.bfloat16),
        in_specs=[
            pl.BlockSpec(memory_space=pltpu.SMEM),
            pl.BlockSpec(memory_space=pltpu.VMEM),
            pl.BlockSpec(memory_space=pltpu.VMEM),
            pl.BlockSpec(memory_space=pltpu.VMEM),
        ],
        out_specs=pl.BlockSpec(memory_space=pltpu.VMEM),
        scratch_shapes=[pltpu.SMEM((2 * SLOTS,), jnp.int32)],
        compiler_params=pltpu.CompilerParams(vmem_limit_bytes=24 * 1024 * 1024),
        name="attend",
    )(span_table, doc_ids.reshape(KEYS // 128, 128), q, kv.reshape(2, 2 * SLOTS, SPAN, HEAD))


CHUNK = 512
CHUNKS = 8


def project_kernel(
    o_ref, w_ref, out_ref, attn, weight, share, theirs, w_sem, b_send, b_recv, s_send, s_recv
):
    cp, core, x, z, y, band, cross = place()
    for n in range(CHUNKS):
        pltpu.make_async_copy(w_ref.at[:, pl.ds(n * CHUNK, CHUNK)], weight.at[n], w_sem.at[n]).start()
    enter_group(x, z, y, core, ())
    zs = z + cross * (3 - 2 * z)
    copies = []
    for dy in range(4):
        yy = (y + dy) % 4
        src, dst = o_ref.at[yy], attn.at[y]
        copy = pltpu.make_async_remote_copy(
            src_ref=src,
            dst_ref=dst,
            send_sem=b_send.at[dy],
            recv_sem=b_recv,
            device_id=(chip(x, zs, yy), band),
            device_id_type=MESH,
        )
        copies.append(copy)
        if dy == 0:

            @pl.when(cross == 0)
            def _():
                pltpu.make_async_copy(src, dst, b_recv).start()

            @pl.when(cross != 0)
            def _():
                copy.start()
        else:
            copy.start()
    pltpu.make_async_copy(attn, attn, b_recv).wait()
    mine = pl.ds(pl.multiple_of(core * SPAN, SPAN), SPAN)
    yours = pl.ds(pl.multiple_of((1 - core) * SPAN, SPAN), SPAN)

    def give(n):
        return pltpu.make_async_remote_copy(
            src_ref=share.at[n, yours],
            dst_ref=theirs.at[n],
            send_sem=s_send.at[n],
            recv_sem=s_recv.at[n],
            device_id=(cp, 1 - core),
            device_id_type=MESH,
        )

    def multiply(n, carry):
        pltpu.make_async_copy(weight.at[n], weight.at[n], w_sem.at[n]).wait()
        acc = jnp.dot(attn[0], weight[n, 0:GROUP, :], preferred_element_type=jnp.float32)
        for k in range(1, 4):
            acc += jnp.dot(attn[k], weight[n, k * GROUP : (k + 1) * GROUP, :], preferred_element_type=jnp.float32)
        share[n] = acc.astype(jnp.bfloat16)
        give(n).start()
        return carry

    lax.fori_loop(0, CHUNKS, multiply, 0)

    def add(n, carry):
        give(n).wait()
        cols = pl.ds(pl.multiple_of(n * CHUNK, CHUNK), CHUNK)
        total = share[n, mine, :].astype(jnp.float32) + theirs[n].astype(jnp.float32)
        out_ref[:, cols] = total.astype(jnp.bfloat16)
        return carry

    lax.fori_loop(0, CHUNKS, add, 0)
    for dy, copy in enumerate(copies):
        if dy == 0:

            @pl.when(cross != 0)
            def _():
                copy.wait_send()
        else:
            copy.wait_send()


def project(o, weight):
    return pl.pallas_call(
        project_kernel,
        out_shape=jax.ShapeDtypeStruct((SPAN, 4096), jnp.bfloat16),
        in_specs=[pl.BlockSpec(memory_space=pl.ANY), pl.BlockSpec(memory_space=pltpu.HBM)],
        out_specs=pl.BlockSpec(memory_space=pltpu.VMEM),
        scratch_shapes=[
            pltpu.VMEM((4, ROWS, GROUP), jnp.bfloat16),
            pltpu.VMEM((CHUNKS, 2048, CHUNK), jnp.bfloat16),
            pltpu.VMEM((CHUNKS, ROWS, CHUNK), jnp.bfloat16),
            pltpu.VMEM((CHUNKS, SPAN, CHUNK), jnp.bfloat16),
            pltpu.SemaphoreType.DMA((CHUNKS,)),
            pltpu.SemaphoreType.DMA((4,)),
            pltpu.SemaphoreType.DMA,
            pltpu.SemaphoreType.DMA((CHUNKS,)),
            pltpu.SemaphoreType.DMA((CHUNKS,)),
        ],
        compiler_params=pltpu.CompilerParams(
            collective_id=1, has_side_effects=True, vmem_limit_bytes=32 * 1024 * 1024
        ),
        name="project",
    )(o, weight)


def local(queries, keys, values, span_table, doc_ids, out_weight):
    q, kv = spread(queries, keys, values)
    o = attend(span_table, doc_ids, q, kv)
    return project(o, out_weight)


def solution(mesh):
    return jax.shard_map(
        local,
        mesh=mesh,
        in_specs=(P("cp", "hd"), P("cp", "hd"), P("cp", "hd"), P(), P(), P("hd", None)),
        out_specs=P(("cp", "hd"), None),
        check_vma=False,
    )
```

```python
import jax
import jax.numpy as jnp
from jax import lax
from jax.experimental import pallas as pl
from jax.experimental.pallas import tpu as pltpu
from jax.sharding import PartitionSpec as P

HEAD = 128
SPAN = 96
ROWS = 192
GROUP = 512
SLOTS = 64
KEYS = 12288
BLOCK = 384
MESH = pl.DeviceIdType.MESH
NEG = -1e30


def place():
    cp = lax.axis_index("cp")
    core = lax.axis_index("hd")
    x = cp // 16
    z = (cp // 4) % 4
    y = cp % 4
    band = z // 2
    cross = (band - core) * (band - core)
    return cp, core, x, z, y, band, cross


def chip(x, z, y):
    return x * 16 + z * 4 + y


def enter_group(x, z, y, core, others):
    barrier = pltpu.get_barrier_semaphore()
    count = 0
    for dz in range(2):
        zz = z if dz == 0 else 3 - z
        for dy in range(4):
            for dc in range(2):
                if dz + dy + dc == 0:
                    continue
                target = (chip(x, zz, (y + dy) % 4), (core + dc) % 2)
                pl.semaphore_signal(barrier, inc=1, device_id=target, device_id_type=MESH)
                count += 1
    for target in others:
        pl.semaphore_signal(barrier, inc=1, device_id=target, device_id_type=MESH)
        count += 1
    pl.semaphore_wait(barrier, count)


def spread_kernel(
    q_ref, k_ref, v_ref, qr_ref, kv_ref, ex_send, ex_recv, q_send, q_recv, ag_send, ag_recv, dd_send, dd_recv
):
    cp, core, x, z, y, band, cross = place()
    zo = 3 - z
    za = z + 1 - 2 * (z % 2)
    zao = 3 - za
    xr, xl, xo = (x + 1) % 4, (x + 3) % 4, (x + 2) % 4
    right = (chip(xr, z, y), core)
    left = (chip(xl, z, y), core)
    across = (chip(x, za, y), core)
    twin = (cp, 1 - core)
    enter_group(x, z, y, core, (right, left, across))

    zt = z + cross * (3 - 2 * z)
    finish = []

    def push(src, dst, device, send_sem, recv_sem, own):
        copy = pltpu.make_async_remote_copy(
            src_ref=src, dst_ref=dst, send_sem=send_sem, recv_sem=recv_sem, device_id=device, device_id_type=MESH
        )
        if own is None:
            copy.start()
            finish.append((None, copy))
            return

        @pl.when(own)
        def _():
            pltpu.make_async_copy(src, dst, recv_sem).start()

        @pl.when(jnp.logical_not(own))
        def _():
            copy.start()

        finish.append((own, copy))

    for dy in range(4):
        yy = (y + dy) % 4
        home = chip(x, zt, yy)
        cols = pl.ds(pl.multiple_of(yy * HEAD, HEAD), HEAD)
        for t, ref in enumerate((k_ref, v_ref)):
            own = (cross + jnp.abs(core - t) == 0) if dy == 0 else None
            push(
                ref.at[:, cols],
                kv_ref.at[t, cp],
                (home, t),
                ex_send.at[dy * 2 + t],
                ex_recv.at[cross],
                own,
            )
    keeper = core + cross * (1 - 2 * core)
    for dy in range(4):
        yy = (y + dy) % 4
        cols = pl.ds(pl.multiple_of(yy * GROUP, GROUP), GROUP)
        own = (cross == 0) if dy == 0 else None
        push(
            q_ref.at[:, cols],
            qr_ref.at[y],
            (chip(x, zt, yy), keeper),
            q_send.at[dy],
            q_recv,
            own,
        )

    def part(t, xs, zs):
        return kv_ref.at[t, pl.ds(xs * 16 + zs * 4, 4)]

    def arrive(t, xs, zs, sem):
        ref = part(t, xs, zs)
        pltpu.make_async_copy(ref, ref, sem).wait()

    def run(t, steps):
        sends = []
        for kind, xs, zs, targets in steps:
            if kind == "own":
                arrive(t, xs, zs, ex_recv.at[0])
            elif kind == "pair":
                arrive(t, xs, zs, ex_recv.at[1])
            else:
                arrive(t, xs, zs, ag_recv.at[xs * 4 + zs])
            for device in targets:
                copy = pltpu.make_async_remote_copy(
                    src_ref=part(t, xs, zs),
                    dst_ref=part(t, xs, zs),
                    send_sem=ag_send.at[len(sends)],
                    recv_sem=ag_recv.at[xs * 4 + zs],
                    device_id=device,
                    device_id_type=MESH,
                )
                copy.start()
                sends.append(copy)
            copy = pltpu.make_async_remote_copy(
                src_ref=part(t, xs, zs),
                dst_ref=part(t, xs, zs),
                send_sem=dd_send.at[xs * 4 + zs],
                recv_sem=dd_recv.at[xs * 4 + zs],
                device_id=twin,
                device_id_type=MESH,
            )
            copy.start()
        for copy in sends:
            copy.wait_send()

    @pl.when(core == 0)
    def _():
        run(
            0,
            (
                ("own", x, z, (across, right, left)),
                ("pair", x, zo, (across, left, right)),
                ("got", x, za, (right, left)),
                ("got", x, zao, (left, right)),
                ("got", xl, z, (right,)),
                ("got", xr, z, ()),
                ("got", xr, zo, (left,)),
                ("got", xl, zo, ()),
                ("got", xl, za, (right,)),
                ("got", xr, za, ()),
                ("got", xr, zao, (left,)),
                ("got", xl, zao, ()),
                ("got", xo, z, ()),
                ("got", xo, zo, ()),
                ("got", xo, za, ()),
                ("got", xo, zao, ()),
            ),
        )

    @pl.when(core == 1)
    def _():
        run(
            1,
            (
                ("own", x, z, (right, left, across)),
                ("pair", x, zo, (left, right, across)),
                ("got", xl, z, (right, across)),
                ("got", xr, z, (across,)),
                ("got", xr, zo, (left, across)),
                ("got", xl, zo, (across,)),
                ("got", x, za, ()),
                ("got", x, zao, ()),
                ("got", xo, z, (across,)),
                ("got", xo, zo, (across,)),
                ("got", xl, za, ()),
                ("got", xr, za, ()),
                ("got", xr, zao, ()),
                ("got", xl, zao, ()),
                ("got", xo, za, ()),
                ("got", xo, zao, ()),
            ),
        )

    for piece in range(16):
        ref = kv_ref.at[1 - core, pl.ds(piece * 4, 4)]
        pltpu.make_async_copy(ref, ref, dd_recv.at[piece]).wait()
        ref = kv_ref.at[core, pl.ds(piece * 4, 4)]
        pltpu.make_async_copy(ref, ref, dd_send.at[piece]).wait()
    pltpu.make_async_copy(qr_ref, qr_ref, q_recv).wait()
    for own, copy in finish:
        if own is None:
            copy.wait_send()
        else:

            @pl.when(jnp.logical_not(own))
            def _():
                copy.wait_send()


def spread(queries, keys, values):
    return pl.pallas_call(
        spread_kernel,
        out_shape=(
            jax.ShapeDtypeStruct((4, ROWS, GROUP), jnp.bfloat16),
            jax.ShapeDtypeStruct((2, SLOTS, ROWS, HEAD), jnp.bfloat16),
        ),
        in_specs=[pl.BlockSpec(memory_space=pltpu.HBM)] * 3,
        out_specs=[pl.BlockSpec(memory_space=pltpu.VMEM)] * 2,
        scratch_shapes=[
            pltpu.SemaphoreType.DMA((8,)),
            pltpu.SemaphoreType.DMA((2,)),
            pltpu.SemaphoreType.DMA((4,)),
            pltpu.SemaphoreType.DMA,
            pltpu.SemaphoreType.DMA((14,)),
            pltpu.SemaphoreType.DMA((16,)),
            pltpu.SemaphoreType.DMA((16,)),
            pltpu.SemaphoreType.DMA((16,)),
        ],
        compiler_params=pltpu.CompilerParams(
            collective_id=0, has_side_effects=True, vmem_limit_bytes=8 * 1024 * 1024
        ),
        cost_estimate=pl.CostEstimate(flops=20_000_000_000, bytes_accessed=40_000_000, transcendentals=0),
        name="spread",
    )(queries, keys, values)


WIDTH = 4 * SPAN
ITEMS = 96
UNROLL = 4
HUGE = 2.0**100
FACTOR = HEAD ** (-0.5) * 1.4426950408889634


def attend_kernel(
    span_ref, doc_ref, q_ref, kv_ref, o_ref, slot_ref, item_q, item_low, item_first, qa_ref, s_ref, p_ref, acc_ref
):
    cp, core, x, z, y, band, cross = place()
    zs = z + cross * (3 - 2 * z)

    def invert(slot, carry):
        slot_ref[span_ref[slot]] = slot
        return carry

    lax.fori_loop(0, 2 * SLOTS, invert, 0, unroll=8)
    docs = doc_ref[...]
    starts = [jnp.int32(0)]
    starts += [jnp.sum((docs < d).astype(jnp.float32)).astype(jnp.int32) for d in range(1, 8)]
    ends = starts[1:] + [jnp.int32(KEYS)]
    lane = lax.broadcasted_iota(jnp.int32, (1, HEAD), 1)
    start = jnp.where(lane == 104, -KEYS, KEYS)
    end = jnp.zeros((1, HEAD), jnp.int32)
    for d in range(8):
        start = jnp.where(lane == d, starts[d], start)
        end = jnp.where(lane == d, ends[d], end)

    def record(at, index, low, first):
        item_q[at] = index
        item_low[at] = low
        item_first[at] = first

    def plan(index, at):
        span = span_ref[2 * chip(x, zs, index // 2) + index % 2]
        first = span * SPAN
        row = lax.broadcasted_iota(jnp.int32, (SPAN, HEAD), 0)
        col = lax.broadcasted_iota(jnp.int32, (SPAN, HEAD), 1)
        pos = row + first
        hidden = jnp.logical_not((pos >= start) & (pos < end)) & (col < 8)
        hidden = hidden | ((col >= 8) & (col < 104) & (col - 8 > row)) | (col == 104)
        qa_ref[index] = jnp.where(hidden, -HUGE, 0.0).astype(jnp.bfloat16)
        acc_ref[index] = jnp.zeros((HEAD + 16, WIDTH), jnp.float32)
        lowest = jnp.int32(0)
        for d in range(1, 8):
            lowest = jnp.where(first >= starts[d], starts[d], lowest)
        blocks = (first + SPAN - lowest + BLOCK - 1) // BLOCK

        def add(step, at):
            record(
                at,
                index,
                span - 3 - 4 * step,
                jnp.where(step == 0, 1, 0),
            )
            return at + 1

        return lax.fori_loop(0, blocks, add, at)

    for at in range(2):
        record(at, 8, 0, 0)
    total = lax.fori_loop(0, 8, plan, jnp.int32(2))
    for at in range(UNROLL + 2):
        record(total + at, 8, 0, 0)
    s_ref[1] = jnp.zeros((BLOCK, WIDTH), jnp.float32)
    p_ref[0] = jnp.zeros((BLOCK, WIDTH), jnp.bfloat16)
    acc_ref[8] = jnp.zeros((HEAD + 16, WIDTH), jnp.float32)
    qa_ref[8] = jnp.zeros((SPAN, HEAD), jnp.bfloat16)
    row = lax.broadcasted_iota(jnp.int32, (BLOCK, HEAD), 0)
    col = lax.broadcasted_iota(jnp.int32, (BLOCK, HEAD), 1)
    corner = jnp.where(row >= BLOCK - SPAN, row - (BLOCK - SPAN) + 8, -1)

    def fetch(which, low):
        slots = [slot_ref[jnp.maximum(low + j, 0)] for j in range(4)]
        return jnp.concatenate([kv_ref[which, slot] for slot in slots], axis=0)

    def step(at, parity, state):
        best, fade = state
        low = item_low[at + 2]
        base = low * SPAN
        seen = (row >= start - base) & (row < end - base)
        seen = seen | (corner + (1 - item_first[at + 2]) * 4096 == col)
        extra = jnp.where(seen, 1.0, 0.0).astype(jnp.bfloat16)
        keys = jnp.concatenate([fetch(0, low), extra], axis=1)
        index = item_q[at + 2]
        source = jnp.minimum(index, 7)
        rows = pl.ds(pl.multiple_of((source % 2) * SPAN, SPAN), SPAN)
        q = q_ref[source // 2, rows, :]
        q = jnp.concatenate([q[:, h * HEAD : (h + 1) * HEAD] for h in range(4)], axis=0)
        q = jnp.concatenate([q, jnp.concatenate([qa_ref[index]] * 4, axis=0)], axis=1)
        s_ref[parity] = lax.dot_general(keys, q, (((1,), (1,)), ((), ())), preferred_element_type=jnp.float32)

        s = s_ref[1 - parity]
        best = jnp.where(item_first[at + 1] == 1, NEG, best)
        new = jnp.maximum(best, jnp.max(s, axis=0, keepdims=True))
        p_ref[1 - parity] = jnp.exp2((s - new) * FACTOR).astype(jnp.bfloat16)

        v = fetch(1, item_low[at])
        v = jnp.concatenate([v.T, jnp.ones((16, BLOCK), jnp.bfloat16)], axis=0)
        index = item_q[at]
        acc_ref[index] = acc_ref[index] * fade + jnp.dot(v, p_ref[parity], preferred_element_type=jnp.float32)
        return new, jnp.exp2((best - new) * FACTOR)

    def several(turn, state):
        for k in range(UNROLL):
            state = step(UNROLL * turn + k, k % 2, state)
        return state

    lax.fori_loop(
        0,
        (total + UNROLL - 1) // UNROLL,
        several,
        (jnp.full((1, WIDTH), NEG, jnp.float32), jnp.zeros((1, WIDTH), jnp.float32)),
    )

    def finish(index, carry):
        rows = pl.ds(pl.multiple_of((index % 2) * SPAN, SPAN), SPAN)
        out = (acc_ref[index, 0:HEAD] / acc_ref[index, HEAD : HEAD + 1]).T.astype(jnp.bfloat16)
        for h in range(4):
            o_ref[index // 2, rows, h * HEAD : (h + 1) * HEAD] = out[h * SPAN : (h + 1) * SPAN]
        return carry

    lax.fori_loop(0, 8, finish, 0)


def attend(span_table, doc_ids, q, kv):
    return pl.pallas_call(
        attend_kernel,
        out_shape=jax.ShapeDtypeStruct((4, ROWS, GROUP), jnp.bfloat16),
        in_specs=[
            pl.BlockSpec(memory_space=pltpu.SMEM),
            pl.BlockSpec(memory_space=pltpu.VMEM),
            pl.BlockSpec(memory_space=pltpu.VMEM),
            pl.BlockSpec(memory_space=pltpu.VMEM),
        ],
        out_specs=pl.BlockSpec(memory_space=pltpu.VMEM),
        scratch_shapes=[
            pltpu.SMEM((2 * SLOTS,), jnp.int32),
            pltpu.SMEM((ITEMS,), jnp.int32),
            pltpu.SMEM((ITEMS,), jnp.int32),
            pltpu.SMEM((ITEMS,), jnp.int32),
            pltpu.VMEM((9, SPAN, HEAD), jnp.bfloat16),
            pltpu.VMEM((2, BLOCK, WIDTH), jnp.float32),
            pltpu.VMEM((2, BLOCK, WIDTH), jnp.bfloat16),
            pltpu.VMEM((9, HEAD + 16, WIDTH), jnp.float32),
        ],
        compiler_params=pltpu.CompilerParams(vmem_limit_bytes=24 * 1024 * 1024),
        name="attend",
    )(span_table, doc_ids.reshape(KEYS // 128, 128), q, kv.reshape(2, 2 * SLOTS, SPAN, HEAD))


CHUNK = 512
CHUNKS = 8


def project_kernel(
    o_ref, w_ref, out_ref, attn, weight, share, theirs, w_sem, b_send, b_recv, s_send, s_recv
):
    cp, core, x, z, y, band, cross = place()
    for n in range(CHUNKS):
        pltpu.make_async_copy(w_ref.at[:, pl.ds(n * CHUNK, CHUNK)], weight.at[n], w_sem.at[n]).start()
    enter_group(x, z, y, core, ())
    zs = z + cross * (3 - 2 * z)
    copies = []
    for dy in range(4):
        yy = (y + dy) % 4
        src, dst = o_ref.at[yy], attn.at[y]
        copy = pltpu.make_async_remote_copy(
            src_ref=src,
            dst_ref=dst,
            send_sem=b_send.at[dy],
            recv_sem=b_recv,
            device_id=(chip(x, zs, yy), band),
            device_id_type=MESH,
        )
        copies.append(copy)
        if dy == 0:

            @pl.when(cross == 0)
            def _():
                pltpu.make_async_copy(src, dst, b_recv).start()

            @pl.when(cross != 0)
            def _():
                copy.start()
        else:
            copy.start()
    pltpu.make_async_copy(attn, attn, b_recv).wait()
    mine = pl.ds(pl.multiple_of(core * SPAN, SPAN), SPAN)
    yours = pl.ds(pl.multiple_of((1 - core) * SPAN, SPAN), SPAN)

    def give(n):
        return pltpu.make_async_remote_copy(
            src_ref=share.at[n, yours],
            dst_ref=theirs.at[n],
            send_sem=s_send.at[n],
            recv_sem=s_recv.at[n],
            device_id=(cp, 1 - core),
            device_id_type=MESH,
        )

    def multiply(n, carry):
        pltpu.make_async_copy(weight.at[n], weight.at[n], w_sem.at[n]).wait()
        acc = jnp.dot(attn[0], weight[n, 0:GROUP, :], preferred_element_type=jnp.float32)
        for k in range(1, 4):
            acc += jnp.dot(attn[k], weight[n, k * GROUP : (k + 1) * GROUP, :], preferred_element_type=jnp.float32)
        share[n] = acc.astype(jnp.bfloat16)
        give(n).start()
        return carry

    lax.fori_loop(0, CHUNKS, multiply, 0)

    def add(n, carry):
        give(n).wait()
        cols = pl.ds(pl.multiple_of(n * CHUNK, CHUNK), CHUNK)
        total = share[n, mine, :].astype(jnp.float32) + theirs[n].astype(jnp.float32)
        out_ref[:, cols] = total.astype(jnp.bfloat16)
        return carry

    lax.fori_loop(0, CHUNKS, add, 0)
    for dy, copy in enumerate(copies):
        if dy == 0:

            @pl.when(cross != 0)
            def _():
                copy.wait_send()
        else:
            copy.wait_send()


def project(o, weight):
    return pl.pallas_call(
        project_kernel,
        out_shape=jax.ShapeDtypeStruct((SPAN, 4096), jnp.bfloat16),
        in_specs=[pl.BlockSpec(memory_space=pl.ANY), pl.BlockSpec(memory_space=pltpu.HBM)],
        out_specs=pl.BlockSpec(memory_space=pltpu.VMEM),
        scratch_shapes=[
            pltpu.VMEM((4, ROWS, GROUP), jnp.bfloat16),
            pltpu.VMEM((CHUNKS, 2048, CHUNK), jnp.bfloat16),
            pltpu.VMEM((CHUNKS, ROWS, CHUNK), jnp.bfloat16),
            pltpu.VMEM((CHUNKS, SPAN, CHUNK), jnp.bfloat16),
            pltpu.SemaphoreType.DMA((CHUNKS,)),
            pltpu.SemaphoreType.DMA((4,)),
            pltpu.SemaphoreType.DMA,
            pltpu.SemaphoreType.DMA((CHUNKS,)),
            pltpu.SemaphoreType.DMA((CHUNKS,)),
        ],
        compiler_params=pltpu.CompilerParams(
            collective_id=1, has_side_effects=True, vmem_limit_bytes=32 * 1024 * 1024
        ),
        name="project",
    )(o, weight)


def local(queries, keys, values, span_table, doc_ids, out_weight):
    far = lambda value: pltpu.with_memory_space_constraint(value, pltpu.HBM)
    q, kv = spread(far(queries), far(keys), far(values))
    o = attend(span_table, doc_ids, q, kv)
    return project(o, far(out_weight))


def solution(mesh):
    return jax.shard_map(
        local,
        mesh=mesh,
        in_specs=(P("cp", "hd"), P("cp", "hd"), P("cp", "hd"), P(), P(), P("hd", None)),
        out_specs=P(("cp", "hd"), None),
        check_vma=False,
    )
```

```python
import jax
import jax.numpy as jnp
from jax import lax
from jax.experimental import pallas as pl
from jax.experimental.pallas import tpu as pltpu
from jax.sharding import PartitionSpec as P

HEAD = 128
SPAN = 96
ROWS = 192
GROUP = 512
SLOTS = 64
KEYS = 12288
BLOCK = 384
MESH = pl.DeviceIdType.MESH
NEG = -1e30


def place():
    cp = lax.axis_index("cp")
    core = lax.axis_index("hd")
    x = cp // 16
    z = (cp // 4) % 4
    y = cp % 4
    band = z // 2
    cross = (band - core) * (band - core)
    return cp, core, x, z, y, band, cross


def chip(x, z, y):
    return x * 16 + z * 4 + y


def enter_group(x, z, y, core, others):
    barrier = pltpu.get_barrier_semaphore()
    count = 0
    for dz in range(2):
        zz = z if dz == 0 else 3 - z
        for dy in range(4):
            for dc in range(2):
                if dz + dy + dc == 0:
                    continue
                target = (chip(x, zz, (y + dy) % 4), (core + dc) % 2)
                pl.semaphore_signal(barrier, inc=1, device_id=target, device_id_type=MESH)
                count += 1
    for target in others:
        pl.semaphore_signal(barrier, inc=1, device_id=target, device_id_type=MESH)
        count += 1
    pl.semaphore_wait(barrier, count)


def spread_kernel(
    q_ref, k_ref, v_ref, qr_ref, kv_ref, ex_send, ex_recv, q_send, q_recv, ag_send, ag_recv, dd_send, dd_recv
):
    cp, core, x, z, y, band, cross = place()
    zo = 3 - z
    za = z + 1 - 2 * (z % 2)
    zao = 3 - za
    xr, xl, xo = (x + 1) % 4, (x + 3) % 4, (x + 2) % 4
    right = (chip(xr, z, y), core)
    left = (chip(xl, z, y), core)
    across = (chip(x, za, y), core)
    twin = (cp, 1 - core)
    enter_group(x, z, y, core, (right, left, across))

    zt = z + cross * (3 - 2 * z)
    finish = []

    def push(src, dst, device, send_sem, recv_sem, own):
        copy = pltpu.make_async_remote_copy(
            src_ref=src, dst_ref=dst, send_sem=send_sem, recv_sem=recv_sem, device_id=device, device_id_type=MESH
        )
        if own is None:
            copy.start()
            finish.append((None, copy))
            return

        @pl.when(own)
        def _():
            pltpu.make_async_copy(src, dst, recv_sem).start()

        @pl.when(jnp.logical_not(own))
        def _():
            copy.start()

        finish.append((own, copy))

    for dy in (0, 1, 3, 2):
        yy = (y + dy) % 4
        home = chip(x, zt, yy)
        cols = pl.ds(pl.multiple_of(yy * HEAD, HEAD), HEAD)
        for t, ref in enumerate((k_ref, v_ref)):
            own = (cross + jnp.abs(core - t) == 0) if dy == 0 else None
            push(
                ref.at[:, cols],
                kv_ref.at[t, cp],
                (home, t),
                ex_send.at[dy * 2 + t],
                ex_recv.at[4 * cross + y],
                own,
            )
    keeper = core + cross * (1 - 2 * core)
    for dy in (0, 1, 3, 2):
        yy = (y + dy) % 4
        cols = pl.ds(pl.multiple_of(yy * GROUP, GROUP), GROUP)
        own = (cross == 0) if dy == 0 else None
        push(
            q_ref.at[:, cols],
            qr_ref.at[y],
            (chip(x, zt, yy), keeper),
            q_send.at[dy],
            q_recv,
            own,
        )

    def part(t, xs, zs):
        return kv_ref.at[t, pl.ds(xs * 16 + zs * 4, 4)]

    def arrive(ref, sem):
        pltpu.make_async_copy(ref, ref, sem).wait()

    def run(t, order, steps):
        sends = []

        def send(ref, device, piece):
            copy = pltpu.make_async_remote_copy(
                src_ref=ref,
                dst_ref=ref,
                send_sem=ag_send.at[len(sends)],
                recv_sem=ag_recv.at[piece],
                device_id=device,
                device_id_type=MESH,
            )
            copy.start()
            sends.append(copy)

        def share(xs, zs):
            pltpu.make_async_remote_copy(
                src_ref=part(t, xs, zs),
                dst_ref=part(t, xs, zs),
                send_sem=dd_send.at[xs * 4 + zs],
                recv_sem=dd_recv.at[xs * 4 + zs],
                device_id=twin,
                device_id_type=MESH,
            ).start()

        for pair, dy in ((0, 0), (1, 0), (0, 3), (0, 1), (1, 3), (0, 2), (1, 1), (1, 2)):
            ys = (y + dy) % 4
            zs = zo if pair else z
            ref = kv_ref.at[t, chip(x, zs, ys)]
            arrive(ref, ex_recv.at[4 * pair + ys])
            for device in order[pair]:
                send(ref, device, x * 4 + zs)
        share(x, z)
        share(x, zo)
        for xs, zs, targets in steps:
            arrive(part(t, xs, zs), ag_recv.at[xs * 4 + zs])
            for device in targets:
                send(part(t, xs, zs), device, xs * 4 + zs)
            share(xs, zs)
        for copy in sends:
            copy.wait_send()

    @pl.when(core == 0)
    def _():
        run(
            0,
            ((across, right, left), (across, left, right)),
            (
                (x, za, (right, left)),
                (x, zao, (left, right)),
                (xl, z, (right,)),
                (xr, z, ()),
                (xr, zo, (left,)),
                (xl, zo, ()),
                (xl, za, (right,)),
                (xr, za, ()),
                (xr, zao, (left,)),
                (xl, zao, ()),
                (xo, z, ()),
                (xo, zo, ()),
                (xo, za, ()),
                (xo, zao, ()),
            ),
        )

    @pl.when(core == 1)
    def _():
        run(
            1,
            ((right, left, across), (left, right, across)),
            (
                (xl, z, (right, across)),
                (xr, zo, (left, across)),
                (xr, z, (across,)),
                (xl, zo, (across,)),
                (x, za, ()),
                (x, zao, ()),
                (xo, z, (across,)),
                (xo, zo, (across,)),
                (xl, za, ()),
                (xr, zao, ()),
                (xr, za, ()),
                (xl, zao, ()),
                (xo, za, ()),
                (xo, zao, ()),
            ),
        )

    for piece in range(16):
        ref = kv_ref.at[1 - core, pl.ds(piece * 4, 4)]
        pltpu.make_async_copy(ref, ref, dd_recv.at[piece]).wait()
        ref = kv_ref.at[core, pl.ds(piece * 4, 4)]
        pltpu.make_async_copy(ref, ref, dd_send.at[piece]).wait()
    pltpu.make_async_copy(qr_ref, qr_ref, q_recv).wait()
    for own, copy in finish:
        if own is None:
            copy.wait_send()
        else:

            @pl.when(jnp.logical_not(own))
            def _():
                copy.wait_send()


def spread(queries, keys, values):
    return pl.pallas_call(
        spread_kernel,
        out_shape=(
            jax.ShapeDtypeStruct((4, ROWS, GROUP), jnp.bfloat16),
            jax.ShapeDtypeStruct((2, SLOTS, ROWS, HEAD), jnp.bfloat16),
        ),
        in_specs=[pl.BlockSpec(memory_space=pltpu.HBM)] * 3,
        out_specs=[pl.BlockSpec(memory_space=pltpu.VMEM)] * 2,
        scratch_shapes=[
            pltpu.SemaphoreType.DMA((8,)),
            pltpu.SemaphoreType.DMA((8,)),
            pltpu.SemaphoreType.DMA((4,)),
            pltpu.SemaphoreType.DMA,
            pltpu.SemaphoreType.DMA((32,)),
            pltpu.SemaphoreType.DMA((16,)),
            pltpu.SemaphoreType.DMA((16,)),
            pltpu.SemaphoreType.DMA((16,)),
        ],
        compiler_params=pltpu.CompilerParams(
            collective_id=0, has_side_effects=True, vmem_limit_bytes=8 * 1024 * 1024
        ),
        cost_estimate=pl.CostEstimate(flops=20_000_000_000, bytes_accessed=40_000_000, transcendentals=0),
        name="spread",
    )(queries, keys, values)


WIDTH = 4 * SPAN
ITEMS = 96
UNROLL = 4
HUGE = 2.0**100
FACTOR = HEAD ** (-0.5) * 1.4426950408889634


def attend_kernel(
    span_ref, doc_ref, q_ref, kv_ref, o_ref, slot_ref, item_q, item_low, item_first, qa_ref, s_ref, p_ref, acc_ref
):
    cp, core, x, z, y, band, cross = place()
    zs = z + cross * (3 - 2 * z)

    def invert(slot, carry):
        slot_ref[span_ref[slot]] = slot
        return carry

    lax.fori_loop(0, 2 * SLOTS, invert, 0, unroll=8)
    docs = doc_ref[...]
    starts = [jnp.int32(0)]
    starts += [jnp.sum((docs < d).astype(jnp.float32)).astype(jnp.int32) for d in range(1, 8)]
    ends = starts[1:] + [jnp.int32(KEYS)]
    lane = lax.broadcasted_iota(jnp.int32, (1, HEAD), 1)
    start = jnp.where(lane == 104, -KEYS, KEYS)
    end = jnp.zeros((1, HEAD), jnp.int32)
    for d in range(8):
        start = jnp.where(lane == d, starts[d], start)
        end = jnp.where(lane == d, ends[d], end)

    def record(at, index, low, first):
        item_q[at] = index
        item_low[at] = low
        item_first[at] = first

    def plan(index, at):
        span = span_ref[2 * chip(x, zs, index // 2) + index % 2]
        first = span * SPAN
        row = lax.broadcasted_iota(jnp.int32, (SPAN, HEAD), 0)
        col = lax.broadcasted_iota(jnp.int32, (SPAN, HEAD), 1)
        pos = row + first
        hidden = jnp.logical_not((pos >= start) & (pos < end)) & (col < 8)
        hidden = hidden | ((col >= 8) & (col < 104) & (col - 8 > row)) | (col == 104)
        qa_ref[index] = jnp.where(hidden, -HUGE, 0.0).astype(jnp.bfloat16)
        acc_ref[index] = jnp.zeros((HEAD + 16, WIDTH), jnp.float32)
        lowest = jnp.int32(0)
        for d in range(1, 8):
            lowest = jnp.where(first >= starts[d], starts[d], lowest)
        blocks = (first + SPAN - lowest + BLOCK - 1) // BLOCK

        def add(step, at):
            record(
                at,
                index,
                span - 3 - 4 * step,
                jnp.where(step == 0, 1, 0),
            )
            return at + 1

        return lax.fori_loop(0, blocks, add, at)

    for at in range(2):
        record(at, 8, 0, 0)
    total = lax.fori_loop(0, 8, plan, jnp.int32(2))
    for at in range(UNROLL + 2):
        record(total + at, 8, 0, 0)
    s_ref[1] = jnp.zeros((BLOCK, WIDTH), jnp.float32)
    p_ref[0] = jnp.zeros((BLOCK, WIDTH), jnp.bfloat16)
    acc_ref[8] = jnp.zeros((HEAD + 16, WIDTH), jnp.float32)
    qa_ref[8] = jnp.zeros((SPAN, HEAD), jnp.bfloat16)
    row = lax.broadcasted_iota(jnp.int32, (BLOCK, HEAD), 0)
    col = lax.broadcasted_iota(jnp.int32, (BLOCK, HEAD), 1)
    corner = jnp.where(row >= BLOCK - SPAN, row - (BLOCK - SPAN) + 8, -1)

    def fetch(which, low):
        slots = [slot_ref[jnp.maximum(low + j, 0)] for j in range(4)]
        return jnp.concatenate([kv_ref[which, slot] for slot in slots], axis=0)

    def step(at, parity, state):
        best, fade = state
        low = item_low[at + 2]
        base = low * SPAN
        seen = (row >= start - base) & (row < end - base)
        seen = seen | (corner + (1 - item_first[at + 2]) * 4096 == col)
        extra = jnp.where(seen, 1.0, 0.0).astype(jnp.bfloat16)
        keys = jnp.concatenate([fetch(0, low), extra], axis=1)
        index = item_q[at + 2]
        source = jnp.minimum(index, 7)
        rows = pl.ds(pl.multiple_of((source % 2) * SPAN, SPAN), SPAN)
        q = q_ref[source // 2, rows, :]
        q = jnp.concatenate([q[:, h * HEAD : (h + 1) * HEAD] for h in range(4)], axis=0)
        q = jnp.concatenate([q, jnp.concatenate([qa_ref[index]] * 4, axis=0)], axis=1)
        s_ref[parity] = lax.dot_general(keys, q, (((1,), (1,)), ((), ())), preferred_element_type=jnp.float32)

        s = s_ref[1 - parity]
        best = jnp.where(item_first[at + 1] == 1, NEG, best)
        new = jnp.maximum(best, jnp.max(s, axis=0, keepdims=True))
        p_ref[1 - parity] = jnp.exp2((s - new) * FACTOR).astype(jnp.bfloat16)

        v = fetch(1, item_low[at])
        v = jnp.concatenate([v.T, jnp.ones((16, BLOCK), jnp.bfloat16)], axis=0)
        index = item_q[at]
        acc_ref[index] = acc_ref[index] * fade + jnp.dot(v, p_ref[parity], preferred_element_type=jnp.float32)
        return new, jnp.exp2((best - new) * FACTOR)

    def several(turn, state):
        for k in range(UNROLL):
            state = step(UNROLL * turn + k, k % 2, state)
        return state

    lax.fori_loop(
        0,
        (total + UNROLL - 1) // UNROLL,
        several,
        (jnp.full((1, WIDTH), NEG, jnp.float32), jnp.zeros((1, WIDTH), jnp.float32)),
    )

    def finish(index, carry):
        rows = pl.ds(pl.multiple_of((index % 2) * SPAN, SPAN), SPAN)
        out = (acc_ref[index, 0:HEAD] / acc_ref[index, HEAD : HEAD + 1]).T.astype(jnp.bfloat16)
        for h in range(4):
            o_ref[index // 2, rows, h * HEAD : (h + 1) * HEAD] = out[h * SPAN : (h + 1) * SPAN]
        return carry

    lax.fori_loop(0, 8, finish, 0)


def attend(span_table, doc_ids, q, kv):
    return pl.pallas_call(
        attend_kernel,
        out_shape=jax.ShapeDtypeStruct((4, ROWS, GROUP), jnp.bfloat16),
        in_specs=[
            pl.BlockSpec(memory_space=pltpu.SMEM),
            pl.BlockSpec(memory_space=pltpu.VMEM),
            pl.BlockSpec(memory_space=pltpu.VMEM),
            pl.BlockSpec(memory_space=pltpu.VMEM),
        ],
        out_specs=pl.BlockSpec(memory_space=pltpu.VMEM),
        scratch_shapes=[
            pltpu.SMEM((2 * SLOTS,), jnp.int32),
            pltpu.SMEM((ITEMS,), jnp.int32),
            pltpu.SMEM((ITEMS,), jnp.int32),
            pltpu.SMEM((ITEMS,), jnp.int32),
            pltpu.VMEM((9, SPAN, HEAD), jnp.bfloat16),
            pltpu.VMEM((2, BLOCK, WIDTH), jnp.float32),
            pltpu.VMEM((2, BLOCK, WIDTH), jnp.bfloat16),
            pltpu.VMEM((9, HEAD + 16, WIDTH), jnp.float32),
        ],
        compiler_params=pltpu.CompilerParams(vmem_limit_bytes=24 * 1024 * 1024),
        name="attend",
    )(span_table, doc_ids.reshape(KEYS // 128, 128), q, kv.reshape(2, 2 * SLOTS, SPAN, HEAD))


CHUNK = 512
CHUNKS = 8


def project_kernel(
    o_ref, w_ref, out_ref, attn, weight, partial, share, theirs, w_sem, b_send, b_recv, s_send, s_recv
):
    cp, core, x, z, y, band, cross = place()
    for n in range(CHUNKS):
        pltpu.make_async_copy(w_ref.at[:, pl.ds(n * CHUNK, CHUNK)], weight.at[n], w_sem.at[n]).start()
    enter_group(x, z, y, core, ())
    zs = z + cross * (3 - 2 * z)
    copies = []
    for dy in (0, 1, 3, 2):
        yy = (y + dy) % 4
        src, dst = o_ref.at[yy], attn.at[y]
        copy = pltpu.make_async_remote_copy(
            src_ref=src,
            dst_ref=dst,
            send_sem=b_send.at[dy],
            recv_sem=b_recv.at[y],
            device_id=(chip(x, zs, yy), band),
            device_id_type=MESH,
        )
        copies.append(copy)
        if dy == 0:

            @pl.when(cross == 0)
            def _():
                pltpu.make_async_copy(src, dst, b_recv.at[y]).start()

            @pl.when(cross != 0)
            def _():
                copy.start()
        else:
            copy.start()
    mine = pl.ds(pl.multiple_of(core * SPAN, SPAN), SPAN)
    yours = pl.ds(pl.multiple_of((1 - core) * SPAN, SPAN), SPAN)

    def give(n):
        return pltpu.make_async_remote_copy(
            src_ref=share.at[n, yours],
            dst_ref=theirs.at[n],
            send_sem=s_send.at[n],
            recv_sem=s_recv.at[n],
            device_id=(cp, 1 - core),
            device_id_type=MESH,
        )

    def gain(k, n):
        rows = pl.ds(pl.multiple_of(k * GROUP, GROUP), GROUP)
        return jnp.dot(attn[k], weight[n, rows, :], preferred_element_type=jnp.float32)

    for turn, dy in enumerate((0, 3, 1, 2)):
        k = (y + dy) % 4
        pltpu.make_async_copy(attn.at[k], attn.at[k], b_recv.at[k]).wait()

        def multiply(n, carry):
            if turn == 0:
                pltpu.make_async_copy(weight.at[n], weight.at[n], w_sem.at[n]).wait()
                partial[n] = gain(k, n)
            elif turn < 3:
                partial[n] += gain(k, n)
            else:
                share[n] = (partial[n] + gain(k, n)).astype(jnp.bfloat16)
                give(n).start()
            return carry

        lax.fori_loop(0, CHUNKS, multiply, 0)

    def add(n, carry):
        give(n).wait()
        cols = pl.ds(pl.multiple_of(n * CHUNK, CHUNK), CHUNK)
        total = share[n, mine, :].astype(jnp.float32) + theirs[n].astype(jnp.float32)
        out_ref[:, cols] = total.astype(jnp.bfloat16)
        return carry

    lax.fori_loop(0, CHUNKS, add, 0)
    for turn, copy in enumerate(copies):
        if turn == 0:

            @pl.when(cross != 0)
            def _():
                copy.wait_send()
        else:
            copy.wait_send()


def project(o, weight):
    return pl.pallas_call(
        project_kernel,
        out_shape=jax.ShapeDtypeStruct((SPAN, 4096), jnp.bfloat16),
        in_specs=[pl.BlockSpec(memory_space=pl.ANY), pl.BlockSpec(memory_space=pltpu.HBM)],
        out_specs=pl.BlockSpec(memory_space=pltpu.VMEM),
        scratch_shapes=[
            pltpu.VMEM((4, ROWS, GROUP), jnp.bfloat16),
            pltpu.VMEM((CHUNKS, 2048, CHUNK), jnp.bfloat16),
            pltpu.VMEM((CHUNKS, ROWS, CHUNK), jnp.float32),
            pltpu.VMEM((CHUNKS, ROWS, CHUNK), jnp.bfloat16),
            pltpu.VMEM((CHUNKS, SPAN, CHUNK), jnp.bfloat16),
            pltpu.SemaphoreType.DMA((CHUNKS,)),
            pltpu.SemaphoreType.DMA((4,)),
            pltpu.SemaphoreType.DMA((4,)),
            pltpu.SemaphoreType.DMA((CHUNKS,)),
            pltpu.SemaphoreType.DMA((CHUNKS,)),
        ],
        compiler_params=pltpu.CompilerParams(
            collective_id=1, has_side_effects=True, vmem_limit_bytes=32 * 1024 * 1024
        ),
        name="project",
    )(o, weight)


def local(queries, keys, values, span_table, doc_ids, out_weight):
    far = lambda value: pltpu.with_memory_space_constraint(value, pltpu.HBM)
    q, kv = spread(far(queries), far(keys), far(values))
    o = attend(span_table, doc_ids, q, kv)
    return project(o, far(out_weight))


def solution(mesh):
    return jax.shard_map(
        local,
        mesh=mesh,
        in_specs=(P("cp", "hd"), P("cp", "hd"), P("cp", "hd"), P(), P(), P("hd", None)),
        out_specs=P(("cp", "hd"), None),
        check_vma=False,
    )
```

```python
import jax
import jax.numpy as jnp
from jax import lax
from jax.experimental import pallas as pl
from jax.experimental.pallas import tpu as pltpu
from jax.sharding import PartitionSpec as P

HEAD = 128
SPAN = 96
ROWS = 192
GROUP = 512
SLOTS = 64
KEYS = 12288
BLOCK = 384
MESH = pl.DeviceIdType.MESH
NEG = -1e30


def place():
    cp = lax.axis_index("cp")
    core = lax.axis_index("hd")
    x = cp // 16
    z = (cp // 4) % 4
    y = cp % 4
    band = z // 2
    cross = (band - core) * (band - core)
    return cp, core, x, z, y, band, cross


def chip(x, z, y):
    return x * 16 + z * 4 + y


def enter_group(x, z, y, core, others):
    barrier = pltpu.get_barrier_semaphore()
    count = 0
    for dz in range(2):
        zz = z if dz == 0 else 3 - z
        for dy in range(4):
            for dc in range(2):
                if dz + dy + dc == 0:
                    continue
                target = (chip(x, zz, (y + dy) % 4), (core + dc) % 2)
                pl.semaphore_signal(barrier, inc=1, device_id=target, device_id_type=MESH)
                count += 1
    for target in others:
        pl.semaphore_signal(barrier, inc=1, device_id=target, device_id_type=MESH)
        count += 1
    pl.semaphore_wait(barrier, count)


def spread_kernel(
    q_ref, k_ref, v_ref, qr_ref, kv_ref, ex_send, ex_recv, q_send, q_recv, ag_send, ag_recv, dd_send, dd_recv
):
    cp, core, x, z, y, band, cross = place()
    zo = 3 - z
    za = z + 1 - 2 * (z % 2)
    zao = 3 - za
    xr, xl, xo = (x + 1) % 4, (x + 3) % 4, (x + 2) % 4
    right = (chip(xr, z, y), core)
    left = (chip(xl, z, y), core)
    across = (chip(x, za, y), core)
    twin = (cp, 1 - core)
    enter_group(x, z, y, core, (right, left, across))

    zt = z + cross * (3 - 2 * z)
    finish = []

    def push(src, dst, device, send_sem, recv_sem, own):
        copy = pltpu.make_async_remote_copy(
            src_ref=src, dst_ref=dst, send_sem=send_sem, recv_sem=recv_sem, device_id=device, device_id_type=MESH
        )
        if own is None:
            copy.start()
            finish.append((None, copy))
            return

        @pl.when(own)
        def _():
            pltpu.make_async_copy(src, dst, recv_sem).start()

        @pl.when(jnp.logical_not(own))
        def _():
            copy.start()

        finish.append((own, copy))

    for dy in range(4):
        yy = (y + dy) % 4
        home = chip(x, zt, yy)
        cols = pl.ds(pl.multiple_of(yy * HEAD, HEAD), HEAD)
        for t, ref in enumerate((k_ref, v_ref)):
            own = (cross + jnp.abs(core - t) == 0) if dy == 0 else None
            push(
                ref.at[:, cols],
                kv_ref.at[t, cp],
                (home, t),
                ex_send.at[dy * 2 + t],
                ex_recv.at[cross],
                own,
            )
    keeper = core + cross * (1 - 2 * core)

    def query_copy(dy):
        yy = (y + dy) % 4
        cols = pl.ds(pl.multiple_of(yy * GROUP, GROUP), GROUP)
        return pltpu.make_async_remote_copy(
            src_ref=q_ref.at[:, cols],
            dst_ref=qr_ref.at[y],
            send_sem=q_send.at[dy],
            recv_sem=q_recv,
            device_id=(chip(x, zt, yy), keeper),
            device_id_type=MESH,
        )

    def send_queries():
        @pl.when(cross == 0)
        def _():
            cols = pl.ds(pl.multiple_of(y * GROUP, GROUP), GROUP)
            pltpu.make_async_copy(q_ref.at[:, cols], qr_ref.at[y], q_recv).start()

        @pl.when(cross != 0)
        def _():
            query_copy(0).start()

        for dy in range(1, 4):
            query_copy(dy).start()

    def part(t, xs, zs):
        return kv_ref.at[t, pl.ds(xs * 16 + zs * 4, 4)]

    def arrive(t, xs, zs, sem):
        ref = part(t, xs, zs)
        pltpu.make_async_copy(ref, ref, sem).wait()

    def run(t, steps):
        sends = []
        for turn, (kind, xs, zs, targets) in enumerate(steps):
            if turn == 2:
                send_queries()
            if kind == "own":
                arrive(t, xs, zs, ex_recv.at[0])
            elif kind == "pair":
                arrive(t, xs, zs, ex_recv.at[1])
            else:
                arrive(t, xs, zs, ag_recv.at[xs * 4 + zs])
            for device in targets:
                copy = pltpu.make_async_remote_copy(
                    src_ref=part(t, xs, zs),
                    dst_ref=part(t, xs, zs),
                    send_sem=ag_send.at[len(sends)],
                    recv_sem=ag_recv.at[xs * 4 + zs],
                    device_id=device,
                    device_id_type=MESH,
                )
                copy.start()
                sends.append(copy)
            copy = pltpu.make_async_remote_copy(
                src_ref=part(t, xs, zs),
                dst_ref=part(t, xs, zs),
                send_sem=dd_send.at[xs * 4 + zs],
                recv_sem=dd_recv.at[xs * 4 + zs],
                device_id=twin,
                device_id_type=MESH,
            )
            copy.start()
        for copy in sends:
            copy.wait_send()

    @pl.when(core == 0)
    def _():
        run(
            0,
            (
                ("own", x, z, (across, right, left)),
                ("pair", x, zo, (across, left, right)),
                ("got", x, za, (right, left)),
                ("got", x, zao, (left, right)),
                ("got", xl, z, (right,)),
                ("got", xr, z, ()),
                ("got", xr, zo, (left,)),
                ("got", xl, zo, ()),
                ("got", xl, za, (right,)),
                ("got", xr, za, ()),
                ("got", xr, zao, (left,)),
                ("got", xl, zao, ()),
                ("got", xo, z, ()),
                ("got", xo, zo, ()),
                ("got", xo, za, ()),
                ("got", xo, zao, ()),
            ),
        )

    @pl.when(core == 1)
    def _():
        run(
            1,
            (
                ("own", x, z, (right, left, across)),
                ("pair", x, zo, (left, right, across)),
                ("got", xl, z, (right, across)),
                ("got", xr, z, (across,)),
                ("got", xr, zo, (left, across)),
                ("got", xl, zo, (across,)),
                ("got", x, za, ()),
                ("got", x, zao, ()),
                ("got", xo, z, (across,)),
                ("got", xo, zo, (across,)),
                ("got", xl, za, ()),
                ("got", xr, za, ()),
                ("got", xr, zao, ()),
                ("got", xl, zao, ()),
                ("got", xo, za, ()),
                ("got", xo, zao, ()),
            ),
        )

    for piece in range(16):
        ref = kv_ref.at[1 - core, pl.ds(piece * 4, 4)]
        pltpu.make_async_copy(ref, ref, dd_recv.at[piece]).wait()
        ref = kv_ref.at[core, pl.ds(piece * 4, 4)]
        pltpu.make_async_copy(ref, ref, dd_send.at[piece]).wait()
    pltpu.make_async_copy(qr_ref, qr_ref, q_recv).wait()

    @pl.when(cross != 0)
    def _():
        query_copy(0).wait_send()

    for dy in range(1, 4):
        query_copy(dy).wait_send()

    for own, copy in finish:
        if own is None:
            copy.wait_send()
        else:

            @pl.when(jnp.logical_not(own))
            def _():
                copy.wait_send()


def spread(queries, keys, values):
    return pl.pallas_call(
        spread_kernel,
        out_shape=(
            jax.ShapeDtypeStruct((4, ROWS, GROUP), jnp.bfloat16),
            jax.ShapeDtypeStruct((2, SLOTS, ROWS, HEAD), jnp.bfloat16),
        ),
        in_specs=[pl.BlockSpec(memory_space=pltpu.HBM)] * 3,
        out_specs=[pl.BlockSpec(memory_space=pltpu.VMEM)] * 2,
        scratch_shapes=[
            pltpu.SemaphoreType.DMA((8,)),
            pltpu.SemaphoreType.DMA((2,)),
            pltpu.SemaphoreType.DMA((4,)),
            pltpu.SemaphoreType.DMA,
            pltpu.SemaphoreType.DMA((14,)),
            pltpu.SemaphoreType.DMA((16,)),
            pltpu.SemaphoreType.DMA((16,)),
            pltpu.SemaphoreType.DMA((16,)),
        ],
        compiler_params=pltpu.CompilerParams(
            collective_id=0, has_side_effects=True, vmem_limit_bytes=8 * 1024 * 1024
        ),
        cost_estimate=pl.CostEstimate(flops=20_000_000_000, bytes_accessed=40_000_000, transcendentals=0),
        name="spread",
    )(queries, keys, values)


WIDTH = 4 * SPAN
ITEMS = 96
UNROLL = 4
HUGE = 2.0**100
FACTOR = HEAD ** (-0.5) * 1.4426950408889634


def attend_kernel(
    span_ref, doc_ref, q_ref, kv_ref, o_ref, slot_ref, item_q, item_low, item_first, qa_ref, s_ref, p_ref, acc_ref
):
    cp, core, x, z, y, band, cross = place()
    zs = z + cross * (3 - 2 * z)

    def invert(slot, carry):
        slot_ref[span_ref[slot]] = slot
        return carry

    lax.fori_loop(0, 2 * SLOTS, invert, 0, unroll=8)
    docs = doc_ref[...]
    starts = [jnp.int32(0)]
    starts += [jnp.sum((docs < d).astype(jnp.float32)).astype(jnp.int32) for d in range(1, 8)]
    ends = starts[1:] + [jnp.int32(KEYS)]
    lane = lax.broadcasted_iota(jnp.int32, (1, HEAD), 1)
    start = jnp.where(lane == 104, -KEYS, KEYS)
    end = jnp.zeros((1, HEAD), jnp.int32)
    for d in range(8):
        start = jnp.where(lane == d, starts[d], start)
        end = jnp.where(lane == d, ends[d], end)

    def record(at, index, low, first):
        item_q[at] = index
        item_low[at] = low
        item_first[at] = first

    row = lax.broadcasted_iota(jnp.int32, (SPAN, HEAD), 0)
    col = lax.broadcasted_iota(jnp.int32, (SPAN, HEAD), 1)
    later = ((col >= 8) & (col < 104) & (col - 8 > row)) | (col == 104)
    later = jnp.where(later, -HUGE, 0.0)
    reach = jnp.where(lane < 8, start, -KEYS)
    limit = jnp.where(lane < 8, end, 2 * KEYS)
    heads = [(begin, begin // SPAN) for begin in starts]

    def plan(index, at):
        span = span_ref[2 * chip(x, zs, index // 2) + index % 2]
        first = span * SPAN
        same = (row >= reach - first) & (row < limit - first)
        qa_ref[index] = jnp.where(same, later, -HUGE).astype(jnp.bfloat16)
        acc_ref[index] = jnp.zeros((HEAD + 16, WIDTH), jnp.float32)
        lowest = jnp.int32(0)
        for begin, head in heads[1:]:
            lowest = jnp.where(first >= begin, head, lowest)
        for turn in range(9):
            record(at + turn, index, span - 3 - 4 * turn, 1 if turn == 0 else 0)
        return at + ((span - lowest + 4) >> 2)

    for at in range(2):
        record(at, 8, 0, 0)
    total = lax.fori_loop(0, 8, plan, jnp.int32(2))
    for at in range(UNROLL + 2):
        record(total + at, 8, 0, 0)
    s_ref[1] = jnp.zeros((BLOCK, WIDTH), jnp.float32)
    p_ref[0] = jnp.zeros((BLOCK, WIDTH), jnp.bfloat16)
    acc_ref[8] = jnp.zeros((HEAD + 16, WIDTH), jnp.float32)
    qa_ref[8] = jnp.zeros((SPAN, HEAD), jnp.bfloat16)
    row = lax.broadcasted_iota(jnp.int32, (BLOCK, HEAD), 0)
    col = lax.broadcasted_iota(jnp.int32, (BLOCK, HEAD), 1)
    corner = jnp.where(row >= BLOCK - SPAN, row - (BLOCK - SPAN) + 8, -1)

    def fetch(which, low):
        slots = [slot_ref[jnp.maximum(low + j, 0)] for j in range(4)]
        return jnp.concatenate([kv_ref[which, slot] for slot in slots], axis=0)

    def step(at, parity, state):
        best, fade = state
        low = item_low[at + 2]
        base = low * SPAN
        seen = (row >= start - base) & (row < end - base)
        seen = seen | (corner + (1 - item_first[at + 2]) * 4096 == col)
        extra = jnp.where(seen, 1.0, 0.0).astype(jnp.bfloat16)
        keys = jnp.concatenate([fetch(0, low), extra], axis=1)
        index = item_q[at + 2]
        source = jnp.minimum(index, 7)
        rows = pl.ds(pl.multiple_of((source % 2) * SPAN, SPAN), SPAN)
        q = q_ref[source // 2, rows, :]
        q = jnp.concatenate([q[:, h * HEAD : (h + 1) * HEAD] for h in range(4)], axis=0)
        q = jnp.concatenate([q, jnp.concatenate([qa_ref[index]] * 4, axis=0)], axis=1)
        s_ref[parity] = lax.dot_general(keys, q, (((1,), (1,)), ((), ())), preferred_element_type=jnp.float32)

        s = s_ref[1 - parity]
        best = jnp.where(item_first[at + 1] == 1, NEG, best)
        new = jnp.maximum(best, jnp.max(s, axis=0, keepdims=True))
        p_ref[1 - parity] = jnp.exp2(s * FACTOR - new * FACTOR).astype(jnp.bfloat16)

        v = fetch(1, item_low[at])
        v = jnp.concatenate([v.T, jnp.ones((16, BLOCK), jnp.bfloat16)], axis=0)
        index = item_q[at]
        acc_ref[index] = acc_ref[index] * fade + jnp.dot(v, p_ref[parity], preferred_element_type=jnp.float32)
        return new, jnp.exp2((best - new) * FACTOR)

    def several(turn, state):
        for k in range(UNROLL):
            state = step(UNROLL * turn + k, k % 2, state)
        return state

    turns = total >> 2
    state = (jnp.full((1, WIDTH), NEG, jnp.float32), jnp.zeros((1, WIDTH), jnp.float32))
    state = lax.fori_loop(0, turns, several, state)

    def couple(turn, state):
        for k in range(2):
            state = step(UNROLL * turns + 2 * turn + k, k, state)
        return state

    lax.fori_loop(0, (total - UNROLL * turns + 1) >> 1, couple, state)

    def finish(index, carry):
        rows = pl.ds(pl.multiple_of((index % 2) * SPAN, SPAN), SPAN)
        out = (acc_ref[index, 0:HEAD] * (1.0 / acc_ref[index, HEAD : HEAD + 1])).T.astype(jnp.bfloat16)
        for h in range(4):
            o_ref[index // 2, rows, h * HEAD : (h + 1) * HEAD] = out[h * SPAN : (h + 1) * SPAN]
        return carry

    lax.fori_loop(0, 8, finish, 0)


def attend(span_table, doc_ids, q, kv):
    return pl.pallas_call(
        attend_kernel,
        out_shape=jax.ShapeDtypeStruct((4, ROWS, GROUP), jnp.bfloat16),
        in_specs=[
            pl.BlockSpec(memory_space=pltpu.SMEM),
            pl.BlockSpec(memory_space=pltpu.VMEM),
            pl.BlockSpec(memory_space=pltpu.VMEM),
            pl.BlockSpec(memory_space=pltpu.VMEM),
        ],
        out_specs=pl.BlockSpec(memory_space=pltpu.VMEM),
        scratch_shapes=[
            pltpu.SMEM((2 * SLOTS,), jnp.int32),
            pltpu.SMEM((ITEMS,), jnp.int32),
            pltpu.SMEM((ITEMS,), jnp.int32),
            pltpu.SMEM((ITEMS,), jnp.int32),
            pltpu.VMEM((9, SPAN, HEAD), jnp.bfloat16),
            pltpu.VMEM((2, BLOCK, WIDTH), jnp.float32),
            pltpu.VMEM((2, BLOCK, WIDTH), jnp.bfloat16),
            pltpu.VMEM((9, HEAD + 16, WIDTH), jnp.float32),
        ],
        compiler_params=pltpu.CompilerParams(vmem_limit_bytes=24 * 1024 * 1024),
        name="attend",
    )(span_table, doc_ids.reshape(KEYS // 128, 128), q, kv.reshape(2, 2 * SLOTS, SPAN, HEAD))


CHUNK = 512
CHUNKS = 8


def project_kernel(
    o_ref, w_ref, out_ref, attn, weight, partial, share, theirs, w_sem, b_send, b_recv, s_send, s_recv
):
    cp, core, x, z, y, band, cross = place()
    for n in range(CHUNKS):
        pltpu.make_async_copy(w_ref.at[:, pl.ds(n * CHUNK, CHUNK)], weight.at[n], w_sem.at[n]).start()
    enter_group(x, z, y, core, ())
    zs = z + cross * (3 - 2 * z)
    copies = []
    for dy in (0, 1, 3, 2):
        yy = (y + dy) % 4
        src, dst = o_ref.at[yy], attn.at[y]
        copy = pltpu.make_async_remote_copy(
            src_ref=src,
            dst_ref=dst,
            send_sem=b_send.at[dy],
            recv_sem=b_recv.at[y],
            device_id=(chip(x, zs, yy), band),
            device_id_type=MESH,
        )
        copies.append(copy)
        if dy == 0:

            @pl.when(cross == 0)
            def _():
                pltpu.make_async_copy(src, dst, b_recv.at[y]).start()

            @pl.when(cross != 0)
            def _():
                copy.start()
        else:
            copy.start()
    mine = pl.ds(pl.multiple_of(core * SPAN, SPAN), SPAN)
    yours = pl.ds(pl.multiple_of((1 - core) * SPAN, SPAN), SPAN)

    def give(n):
        return pltpu.make_async_remote_copy(
            src_ref=share.at[n, yours],
            dst_ref=theirs.at[n],
            send_sem=s_send.at[n],
            recv_sem=s_recv.at[n],
            device_id=(cp, 1 - core),
            device_id_type=MESH,
        )

    def gain(k, n):
        rows = pl.ds(pl.multiple_of(k * GROUP, GROUP), GROUP)
        return jnp.dot(attn[k], weight[n, rows, :], preferred_element_type=jnp.float32)

    for n in range(CHUNKS):
        pltpu.make_async_copy(weight.at[n], weight.at[n], w_sem.at[n]).wait()
    def block(dy):
        return (y + dy) % 4

    def await_block(dy):
        pltpu.make_async_copy(attn.at[block(dy)], attn.at[block(dy)], b_recv.at[block(dy)]).wait()

    for dy in (0, 3, 1):
        await_block(dy)
    for n in range(CHUNKS):
        partial[n] = gain(block(0), n) + gain(block(3), n) + gain(block(1), n)
    await_block(2)
    for n in range(CHUNKS):
        share[n] = (partial[n] + gain(block(2), n)).astype(jnp.bfloat16)
        give(n).start()

    def add(n, carry):
        give(n).wait()
        cols = pl.ds(pl.multiple_of(n * CHUNK, CHUNK), CHUNK)
        total = share[n, mine, :].astype(jnp.float32) + theirs[n].astype(jnp.float32)
        out_ref[:, cols] = total.astype(jnp.bfloat16)
        return carry

    lax.fori_loop(0, CHUNKS, add, 0)
    for turn, copy in enumerate(copies):
        if turn == 0:

            @pl.when(cross != 0)
            def _():
                copy.wait_send()
        else:
            copy.wait_send()


def project(o, weight):
    return pl.pallas_call(
        project_kernel,
        out_shape=jax.ShapeDtypeStruct((SPAN, 4096), jnp.bfloat16),
        in_specs=[pl.BlockSpec(memory_space=pl.ANY), pl.BlockSpec(memory_space=pltpu.HBM)],
        out_specs=pl.BlockSpec(memory_space=pltpu.VMEM),
        scratch_shapes=[
            pltpu.VMEM((4, ROWS, GROUP), jnp.bfloat16),
            pltpu.VMEM((CHUNKS, 2048, CHUNK), jnp.bfloat16),
            pltpu.VMEM((CHUNKS, ROWS, CHUNK), jnp.float32),
            pltpu.VMEM((CHUNKS, ROWS, CHUNK), jnp.bfloat16),
            pltpu.VMEM((CHUNKS, SPAN, CHUNK), jnp.bfloat16),
            pltpu.SemaphoreType.DMA((CHUNKS,)),
            pltpu.SemaphoreType.DMA((4,)),
            pltpu.SemaphoreType.DMA((4,)),
            pltpu.SemaphoreType.DMA((CHUNKS,)),
            pltpu.SemaphoreType.DMA((CHUNKS,)),
        ],
        compiler_params=pltpu.CompilerParams(
            collective_id=1, has_side_effects=True, vmem_limit_bytes=32 * 1024 * 1024
        ),
        name="project",
    )(o, weight)


def local(queries, keys, values, span_table, doc_ids, out_weight):
    far = lambda value: pltpu.with_memory_space_constraint(value, pltpu.HBM)
    q, kv = spread(far(queries), far(keys), far(values))
    o = attend(span_table, doc_ids, q, kv)
    return project(o, far(out_weight))


def solution(mesh):
    return jax.shard_map(
        local,
        mesh=mesh,
        in_specs=(P("cp", "hd"), P("cp", "hd"), P("cp", "hd"), P(), P(), P("hd", None)),
        out_specs=P(("cp", "hd"), None),
        check_vma=False,
    )
```

```python
import jax
import jax.numpy as jnp
from jax import lax
from jax.experimental import pallas as pl
from jax.experimental.pallas import tpu as pltpu
from jax.sharding import PartitionSpec as P

HEAD = 128
SPAN = 96
ROWS = 192
GROUP = 512
SLOTS = 64
KEYS = 12288
BLOCK = 384
MESH = pl.DeviceIdType.MESH
NEG = -1e30


def place():
    cp = lax.axis_index("cp")
    core = lax.axis_index("hd")
    x = cp // 16
    z = (cp // 4) % 4
    y = cp % 4
    band = z // 2
    cross = (band - core) * (band - core)
    return cp, core, x, z, y, band, cross


def chip(x, z, y):
    return x * 16 + z * 4 + y


def enter_group(x, z, y, core, others):
    barrier = pltpu.get_barrier_semaphore()
    count = 0
    for dz in range(2):
        zz = z if dz == 0 else 3 - z
        for dy in range(4):
            for dc in range(2):
                if dz + dy + dc == 0:
                    continue
                target = (chip(x, zz, (y + dy) % 4), (core + dc) % 2)
                pl.semaphore_signal(barrier, inc=1, device_id=target, device_id_type=MESH)
                count += 1
    for target in others:
        pl.semaphore_signal(barrier, inc=1, device_id=target, device_id_type=MESH)
        count += 1
    pl.semaphore_wait(barrier, count)


def spread_kernel(
    q_ref, k_ref, v_ref, qr_ref, kv_ref, ex_send, ex_recv, q_send, q_recv, ag_send, ag_recv, dd_send, dd_recv
):
    cp, core, x, z, y, band, cross = place()
    zo = 3 - z
    za = z + 1 - 2 * (z % 2)
    zao = 3 - za
    xr, xl, xo = (x + 1) % 4, (x + 3) % 4, (x + 2) % 4
    right = (chip(xr, z, y), core)
    left = (chip(xl, z, y), core)
    across = (chip(x, za, y), core)
    twin = (cp, 1 - core)
    enter_group(x, z, y, core, (right, left, across))

    zt = z + cross * (3 - 2 * z)
    finish = []

    def push(src, dst, device, send_sem, recv_sem, own):
        copy = pltpu.make_async_remote_copy(
            src_ref=src, dst_ref=dst, send_sem=send_sem, recv_sem=recv_sem, device_id=device, device_id_type=MESH
        )
        if own is None:
            copy.start()
            finish.append((None, copy))
            return

        @pl.when(own)
        def _():
            pltpu.make_async_copy(src, dst, recv_sem).start()

        @pl.when(jnp.logical_not(own))
        def _():
            copy.start()

        finish.append((own, copy))

    for dy in range(4):
        yy = (y + dy) % 4
        home = chip(x, zt, yy)
        cols = pl.ds(pl.multiple_of(yy * HEAD, HEAD), HEAD)
        for t, ref in enumerate((k_ref, v_ref)):
            own = (cross + jnp.abs(core - t) == 0) if dy == 0 else None
            push(
                ref.at[:, cols],
                kv_ref.at[t, cp],
                (home, t),
                ex_send.at[dy * 2 + t],
                ex_recv.at[cross],
                own,
            )
    keeper = core + cross * (1 - 2 * core)

    def query_copy(dy):
        yy = (y + dy) % 4
        cols = pl.ds(pl.multiple_of(yy * GROUP, GROUP), GROUP)
        return pltpu.make_async_remote_copy(
            src_ref=q_ref.at[:, cols],
            dst_ref=qr_ref.at[y],
            send_sem=q_send.at[dy],
            recv_sem=q_recv,
            device_id=(chip(x, zt, yy), keeper),
            device_id_type=MESH,
        )

    def send_queries():
        @pl.when(cross == 0)
        def _():
            cols = pl.ds(pl.multiple_of(y * GROUP, GROUP), GROUP)
            pltpu.make_async_copy(q_ref.at[:, cols], qr_ref.at[y], q_recv).start()

        @pl.when(cross != 0)
        def _():
            query_copy(0).start()

        for dy in range(1, 4):
            query_copy(dy).start()

    def part(t, xs, zs):
        return kv_ref.at[t, pl.ds(xs * 16 + zs * 4, 4)]

    def arrive(t, xs, zs, sem):
        ref = part(t, xs, zs)
        pltpu.make_async_copy(ref, ref, sem).wait()

    def run(t, steps):
        sends = []
        for turn, (kind, xs, zs, targets) in enumerate(steps):
            if turn == 2:
                send_queries()
            if kind == "own":
                arrive(t, xs, zs, ex_recv.at[0])
            elif kind == "pair":
                arrive(t, xs, zs, ex_recv.at[1])
            else:
                arrive(t, xs, zs, ag_recv.at[xs * 4 + zs])
            for device in targets:
                copy = pltpu.make_async_remote_copy(
                    src_ref=part(t, xs, zs),
                    dst_ref=part(t, xs, zs),
                    send_sem=ag_send.at[len(sends)],
                    recv_sem=ag_recv.at[xs * 4 + zs],
                    device_id=device,
                    device_id_type=MESH,
                )
                copy.start()
                sends.append(copy)
            copy = pltpu.make_async_remote_copy(
                src_ref=part(t, xs, zs),
                dst_ref=part(t, xs, zs),
                send_sem=dd_send.at[xs * 4 + zs],
                recv_sem=dd_recv.at[xs * 4 + zs],
                device_id=twin,
                device_id_type=MESH,
            )
            copy.start()
        for copy in sends:
            copy.wait_send()

    @pl.when(core == 0)
    def _():
        run(
            0,
            (
                ("own", x, z, (across, right, left)),
                ("pair", x, zo, (across, left, right)),
                ("got", x, za, (right, left)),
                ("got", x, zao, (left, right)),
                ("got", xl, z, (right,)),
                ("got", xr, z, ()),
                ("got", xr, zo, (left,)),
                ("got", xl, zo, ()),
                ("got", xl, za, (right,)),
                ("got", xr, za, ()),
                ("got", xr, zao, (left,)),
                ("got", xl, zao, ()),
                ("got", xo, z, ()),
                ("got", xo, zo, ()),
                ("got", xo, za, ()),
                ("got", xo, zao, ()),
            ),
        )

    @pl.when(core == 1)
    def _():
        run(
            1,
            (
                ("own", x, z, (right, left, across)),
                ("pair", x, zo, (left, right, across)),
                ("got", xl, z, (right, across)),
                ("got", xr, z, (across,)),
                ("got", xr, zo, (left, across)),
                ("got", xl, zo, (across,)),
                ("got", x, za, ()),
                ("got", x, zao, ()),
                ("got", xo, z, (across,)),
                ("got", xo, zo, (across,)),
                ("got", xl, za, ()),
                ("got", xr, za, ()),
                ("got", xr, zao, ()),
                ("got", xl, zao, ()),
                ("got", xo, za, ()),
                ("got", xo, zao, ()),
            ),
        )

    for piece in range(16):
        ref = kv_ref.at[1 - core, pl.ds(piece * 4, 4)]
        pltpu.make_async_copy(ref, ref, dd_recv.at[piece]).wait()
        ref = kv_ref.at[core, pl.ds(piece * 4, 4)]
        pltpu.make_async_copy(ref, ref, dd_send.at[piece]).wait()
    pltpu.make_async_copy(qr_ref, qr_ref, q_recv).wait()

    @pl.when(cross != 0)
    def _():
        query_copy(0).wait_send()

    for dy in range(1, 4):
        query_copy(dy).wait_send()

    for own, copy in finish:
        if own is None:
            copy.wait_send()
        else:

            @pl.when(jnp.logical_not(own))
            def _():
                copy.wait_send()


def spread(queries, keys, values):
    return pl.pallas_call(
        spread_kernel,
        out_shape=(
            jax.ShapeDtypeStruct((4, ROWS, GROUP), jnp.bfloat16),
            jax.ShapeDtypeStruct((2, SLOTS, ROWS, HEAD), jnp.bfloat16),
        ),
        in_specs=[pl.BlockSpec(memory_space=pltpu.HBM)] * 3,
        out_specs=[pl.BlockSpec(memory_space=pltpu.VMEM)] * 2,
        scratch_shapes=[
            pltpu.SemaphoreType.DMA((8,)),
            pltpu.SemaphoreType.DMA((2,)),
            pltpu.SemaphoreType.DMA((4,)),
            pltpu.SemaphoreType.DMA,
            pltpu.SemaphoreType.DMA((14,)),
            pltpu.SemaphoreType.DMA((16,)),
            pltpu.SemaphoreType.DMA((16,)),
            pltpu.SemaphoreType.DMA((16,)),
        ],
        compiler_params=pltpu.CompilerParams(
            collective_id=0, has_side_effects=True, vmem_limit_bytes=8 * 1024 * 1024
        ),
        cost_estimate=pl.CostEstimate(flops=20_000_000_000, bytes_accessed=40_000_000, transcendentals=0),
        name="spread",
    )(queries, keys, values)


WIDTH = 4 * SPAN
ITEMS = 96
UNROLL = 8
HUGE = 2.0**100
FACTOR = HEAD ** (-0.5) * 1.4426950408889634


def attend_kernel(
    span_ref, doc_ref, q_ref, kv_ref, o_ref, slot_ref, item_q, item_low, item_first, qa_ref, s_ref, p_ref, acc_ref
):
    cp, core, x, z, y, band, cross = place()
    zs = z + cross * (3 - 2 * z)

    def invert(slot, carry):
        slot_ref[span_ref[slot]] = slot
        return carry

    lax.fori_loop(0, 2 * SLOTS, invert, 0, unroll=8)
    docs = doc_ref[...]
    starts = [jnp.int32(0)]
    starts += [jnp.sum((docs < d).astype(jnp.float32)).astype(jnp.int32) for d in range(1, 8)]
    ends = starts[1:] + [jnp.int32(KEYS)]
    lane = lax.broadcasted_iota(jnp.int32, (1, HEAD), 1)
    start = jnp.where(lane == 104, -KEYS, KEYS)
    end = jnp.zeros((1, HEAD), jnp.int32)
    for d in range(8):
        start = jnp.where(lane == d, starts[d], start)
        end = jnp.where(lane == d, ends[d], end)

    def record(at, index, low, first):
        item_q[at] = index
        item_low[at] = low
        item_first[at] = first

    row = lax.broadcasted_iota(jnp.int32, (SPAN, HEAD), 0)
    col = lax.broadcasted_iota(jnp.int32, (SPAN, HEAD), 1)
    later = ((col >= 8) & (col < 104) & (col - 8 > row)) | (col == 104)
    later = jnp.where(later, -HUGE, 0.0)
    reach = jnp.where(lane < 8, start, -KEYS)
    limit = jnp.where(lane < 8, end, 2 * KEYS)
    heads = [(begin, begin // SPAN) for begin in starts]

    def plan(index, at):
        span = span_ref[2 * chip(x, zs, index // 2) + index % 2]
        first = span * SPAN
        same = (row >= reach - first) & (row < limit - first)
        qa_ref[index] = jnp.where(same, later, -HUGE).astype(jnp.bfloat16)
        acc_ref[index] = jnp.zeros((HEAD + 16, WIDTH), jnp.float32)
        lowest = jnp.int32(0)
        for begin, head in heads[1:]:
            lowest = jnp.where(first >= begin, head, lowest)
        for turn in range(9):
            record(at + turn, index, span - 3 - 4 * turn, 1 if turn == 0 else 0)
        return at + ((span - lowest + 4) >> 2)

    for at in range(2):
        record(at, 8, 0, 0)
    total = lax.fori_loop(0, 8, plan, jnp.int32(2))
    for at in range(UNROLL + 2):
        record(total + at, 8, 0, 0)
    s_ref[1] = jnp.zeros((BLOCK, WIDTH), jnp.float32)
    p_ref[0] = jnp.zeros((BLOCK, WIDTH), jnp.bfloat16)
    acc_ref[8] = jnp.zeros((HEAD + 16, WIDTH), jnp.float32)
    qa_ref[8] = jnp.zeros((SPAN, HEAD), jnp.bfloat16)
    row = lax.broadcasted_iota(jnp.int32, (BLOCK, HEAD), 0)
    col = lax.broadcasted_iota(jnp.int32, (BLOCK, HEAD), 1)
    corner = jnp.where(row >= BLOCK - SPAN, row - (BLOCK - SPAN) + 8, -1)

    def fetch(which, low):
        slots = [slot_ref[jnp.maximum(low + j, 0)] for j in range(4)]
        return jnp.concatenate([kv_ref[which, slot] for slot in slots], axis=0)

    def step(at, parity, state):
        best, fade = state
        low = item_low[at + 2]
        base = low * SPAN
        seen = (row >= start - base) & (row < end - base)
        seen = seen | (corner + (1 - item_first[at + 2]) * 4096 == col)
        extra = jnp.where(seen, 1.0, 0.0).astype(jnp.bfloat16)
        keys = jnp.concatenate([fetch(0, low), extra], axis=1)
        index = item_q[at + 2]
        source = jnp.minimum(index, 7)
        rows = pl.ds(pl.multiple_of((source % 2) * SPAN, SPAN), SPAN)
        q = q_ref[source // 2, rows, :]
        q = jnp.concatenate([q[:, h * HEAD : (h + 1) * HEAD] for h in range(4)], axis=0)
        q = jnp.concatenate([q, jnp.concatenate([qa_ref[index]] * 4, axis=0)], axis=1)
        s_ref[parity] = lax.dot_general(keys, q, (((1,), (1,)), ((), ())), preferred_element_type=jnp.float32)

        s = s_ref[1 - parity]
        best = jnp.where(item_first[at + 1] == 1, NEG, best)
        new = jnp.maximum(best, jnp.max(s, axis=0, keepdims=True))
        p_ref[1 - parity] = jnp.exp2(s * FACTOR - new * FACTOR).astype(jnp.bfloat16)

        v = fetch(1, item_low[at])
        v = jnp.concatenate([v.T, jnp.ones((16, BLOCK), jnp.bfloat16)], axis=0)
        index = item_q[at]
        acc_ref[index] = acc_ref[index] * fade + jnp.dot(v, p_ref[parity], preferred_element_type=jnp.float32)
        return new, jnp.exp2((best - new) * FACTOR)

    def several(turn, state):
        for k in range(UNROLL):
            state = step(UNROLL * turn + k, k % 2, state)
        return state

    turns = total // UNROLL
    state = (jnp.full((1, WIDTH), NEG, jnp.float32), jnp.zeros((1, WIDTH), jnp.float32))
    state = lax.fori_loop(0, turns, several, state)

    def couple(turn, state):
        for k in range(2):
            state = step(UNROLL * turns + 2 * turn + k, k, state)
        return state

    lax.fori_loop(0, (total - UNROLL * turns + 1) >> 1, couple, state)

    def finish(index, carry):
        rows = pl.ds(pl.multiple_of((index % 2) * SPAN, SPAN), SPAN)
        out = (acc_ref[index, 0:HEAD] * (1.0 / acc_ref[index, HEAD : HEAD + 1])).T.astype(jnp.bfloat16)
        for h in range(4):
            o_ref[index // 2, rows, h * HEAD : (h + 1) * HEAD] = out[h * SPAN : (h + 1) * SPAN]
        return carry

    lax.fori_loop(0, 8, finish, 0)


def attend(span_table, doc_ids, q, kv):
    return pl.pallas_call(
        attend_kernel,
        out_shape=jax.ShapeDtypeStruct((4, ROWS, GROUP), jnp.bfloat16),
        in_specs=[
            pl.BlockSpec(memory_space=pltpu.SMEM),
            pl.BlockSpec(memory_space=pltpu.VMEM),
            pl.BlockSpec(memory_space=pltpu.VMEM),
            pl.BlockSpec(memory_space=pltpu.VMEM),
        ],
        out_specs=pl.BlockSpec(memory_space=pltpu.VMEM),
        scratch_shapes=[
            pltpu.SMEM((2 * SLOTS,), jnp.int32),
            pltpu.SMEM((ITEMS,), jnp.int32),
            pltpu.SMEM((ITEMS,), jnp.int32),
            pltpu.SMEM((ITEMS,), jnp.int32),
            pltpu.VMEM((9, SPAN, HEAD), jnp.bfloat16),
            pltpu.VMEM((2, BLOCK, WIDTH), jnp.float32),
            pltpu.VMEM((2, BLOCK, WIDTH), jnp.bfloat16),
            pltpu.VMEM((9, HEAD + 16, WIDTH), jnp.float32),
        ],
        compiler_params=pltpu.CompilerParams(vmem_limit_bytes=24 * 1024 * 1024),
        name="attend",
    )(span_table, doc_ids.reshape(KEYS // 128, 128), q, kv.reshape(2, 2 * SLOTS, SPAN, HEAD))


CHUNK = 512
CHUNKS = 8


def project_kernel(
    o_ref, w_ref, out_ref, attn, weight, partial, share, theirs, w_sem, b_send, b_recv, s_send, s_recv
):
    cp, core, x, z, y, band, cross = place()
    for n in range(CHUNKS):
        pltpu.make_async_copy(w_ref.at[:, pl.ds(n * CHUNK, CHUNK)], weight.at[n], w_sem.at[n]).start()
    zs = z + cross * (3 - 2 * z)
    barrier = pltpu.get_barrier_semaphore()
    pl.semaphore_signal(barrier, inc=1, device_id=(cp, 1 - core), device_id_type=MESH)
    for dy in range(1, 4):
        pl.semaphore_signal(barrier, inc=1, device_id=(chip(x, zs, (y + dy) % 4), band), device_id_type=MESH)

    @pl.when(cross != 0)
    def _():
        pl.semaphore_signal(barrier, inc=1, device_id=(chip(x, zs, y), band), device_id_type=MESH)

    pl.semaphore_wait(barrier, 4 + cross)
    copies = []
    for dy in (0, 1, 3, 2):
        yy = (y + dy) % 4
        src, dst = o_ref.at[yy], attn.at[y]
        copy = pltpu.make_async_remote_copy(
            src_ref=src,
            dst_ref=dst,
            send_sem=b_send.at[dy],
            recv_sem=b_recv.at[y],
            device_id=(chip(x, zs, yy), band),
            device_id_type=MESH,
        )
        copies.append(copy)
        if dy == 0:

            @pl.when(cross == 0)
            def _():
                pltpu.make_async_copy(src, dst, b_recv.at[y]).start()

            @pl.when(cross != 0)
            def _():
                copy.start()
        else:
            copy.start()
    mine = pl.ds(pl.multiple_of(core * SPAN, SPAN), SPAN)
    yours = pl.ds(pl.multiple_of((1 - core) * SPAN, SPAN), SPAN)

    def give(n):
        return pltpu.make_async_remote_copy(
            src_ref=share.at[n, yours],
            dst_ref=theirs.at[n],
            send_sem=s_send.at[n],
            recv_sem=s_recv.at[n],
            device_id=(cp, 1 - core),
            device_id_type=MESH,
        )

    def gain(k, n):
        rows = pl.ds(pl.multiple_of(k * GROUP, GROUP), GROUP)
        return jnp.dot(attn[k], weight[n, rows, :], preferred_element_type=jnp.float32)

    for n in range(CHUNKS):
        pltpu.make_async_copy(weight.at[n], weight.at[n], w_sem.at[n]).wait()
    def block(dy):
        return (y + dy) % 4

    def await_block(dy):
        pltpu.make_async_copy(attn.at[block(dy)], attn.at[block(dy)], b_recv.at[block(dy)]).wait()

    for dy in (0, 3, 1):
        await_block(dy)
    for n in range(CHUNKS):
        partial[n] = gain(block(0), n) + gain(block(3), n) + gain(block(1), n)
    await_block(2)
    for n in range(CHUNKS):
        share[n] = (partial[n] + gain(block(2), n)).astype(jnp.bfloat16)
        give(n).start()

    def add(n, carry):
        give(n).wait()
        cols = pl.ds(pl.multiple_of(n * CHUNK, CHUNK), CHUNK)
        total = share[n, mine, :].astype(jnp.float32) + theirs[n].astype(jnp.float32)
        out_ref[:, cols] = total.astype(jnp.bfloat16)
        return carry

    lax.fori_loop(0, CHUNKS, add, 0)
    for turn, copy in enumerate(copies):
        if turn == 0:

            @pl.when(cross != 0)
            def _():
                copy.wait_send()
        else:
            copy.wait_send()


def project(o, weight):
    return pl.pallas_call(
        project_kernel,
        out_shape=jax.ShapeDtypeStruct((SPAN, 4096), jnp.bfloat16),
        in_specs=[pl.BlockSpec(memory_space=pl.ANY), pl.BlockSpec(memory_space=pltpu.HBM)],
        out_specs=pl.BlockSpec(memory_space=pltpu.VMEM),
        scratch_shapes=[
            pltpu.VMEM((4, ROWS, GROUP), jnp.bfloat16),
            pltpu.VMEM((CHUNKS, 2048, CHUNK), jnp.bfloat16),
            pltpu.VMEM((CHUNKS, ROWS, CHUNK), jnp.float32),
            pltpu.VMEM((CHUNKS, ROWS, CHUNK), jnp.bfloat16),
            pltpu.VMEM((CHUNKS, SPAN, CHUNK), jnp.bfloat16),
            pltpu.SemaphoreType.DMA((CHUNKS,)),
            pltpu.SemaphoreType.DMA((4,)),
            pltpu.SemaphoreType.DMA((4,)),
            pltpu.SemaphoreType.DMA((CHUNKS,)),
            pltpu.SemaphoreType.DMA((CHUNKS,)),
        ],
        compiler_params=pltpu.CompilerParams(
            collective_id=1, has_side_effects=True, vmem_limit_bytes=32 * 1024 * 1024
        ),
        name="project",
    )(o, weight)


def local(queries, keys, values, span_table, doc_ids, out_weight):
    far = lambda value: pltpu.with_memory_space_constraint(value, pltpu.HBM)
    q, kv = spread(far(queries), far(keys), far(values))
    o = attend(span_table, doc_ids, q, kv)
    return project(o, far(out_weight))


def solution(mesh):
    return jax.shard_map(
        local,
        mesh=mesh,
        in_specs=(P("cp", "hd"), P("cp", "hd"), P("cp", "hd"), P(), P(), P("hd", None)),
        out_specs=P(("cp", "hd"), None),
        check_vma=False,
    )
```

```python
import jax
import jax.numpy as jnp
from jax import lax
from jax.experimental import pallas as pl
from jax.experimental.pallas import tpu as pltpu
from jax.sharding import PartitionSpec as P

HEAD = 128
SPAN = 96
ROWS = 192
GROUP = 512
SLOTS = 64
KEYS = 12288
BLOCK = 384
MESH = pl.DeviceIdType.MESH
NEG = -1e30


def place():
    cp = lax.axis_index("cp")
    core = lax.axis_index("hd")
    x = cp // 16
    z = (cp // 4) % 4
    y = cp % 4
    band = z // 2
    cross = (band - core) * (band - core)
    return cp, core, x, z, y, band, cross


def chip(x, z, y):
    return x * 16 + z * 4 + y


def enter_group(x, z, y, core, others):
    barrier = pltpu.get_barrier_semaphore()
    count = 0
    for dz in range(2):
        zz = z if dz == 0 else 3 - z
        for dy in range(4):
            for dc in range(2):
                if dz + dy + dc == 0:
                    continue
                target = (chip(x, zz, (y + dy) % 4), (core + dc) % 2)
                pl.semaphore_signal(barrier, inc=1, device_id=target, device_id_type=MESH)
                count += 1
    for target in others:
        pl.semaphore_signal(barrier, inc=1, device_id=target, device_id_type=MESH)
        count += 1
    pl.semaphore_wait(barrier, count)


def spread_kernel(
    q_ref, k_ref, v_ref, qr_ref, kv_ref, ex_send, ex_recv, q_send, q_recv, ag_send, ag_recv, dd_send, dd_recv
):
    cp, core, x, z, y, band, cross = place()
    zo = 3 - z
    za = z + 1 - 2 * (z % 2)
    zao = 3 - za
    xr, xl, xo = (x + 1) % 4, (x + 3) % 4, (x + 2) % 4
    right = (chip(xr, z, y), core)
    left = (chip(xl, z, y), core)
    across = (chip(x, za, y), core)
    twin = (cp, 1 - core)
    enter_group(x, z, y, core, (right, left, across))

    zt = z + cross * (3 - 2 * z)
    finish = []

    def push(src, dst, device, send_sem, recv_sem, own):
        copy = pltpu.make_async_remote_copy(
            src_ref=src, dst_ref=dst, send_sem=send_sem, recv_sem=recv_sem, device_id=device, device_id_type=MESH
        )
        if own is None:
            copy.start()
            finish.append((None, copy))
            return

        @pl.when(own)
        def _():
            pltpu.make_async_copy(src, dst, recv_sem).start()

        @pl.when(jnp.logical_not(own))
        def _():
            copy.start()

        finish.append((own, copy))

    for dy in range(4):
        yy = (y + dy) % 4
        home = chip(x, zt, yy)
        cols = pl.ds(pl.multiple_of(yy * HEAD, HEAD), HEAD)
        for t, ref in enumerate((k_ref, v_ref)):
            own = (cross + jnp.abs(core - t) == 0) if dy == 0 else None
            push(
                ref.at[:, cols],
                kv_ref.at[t, cp],
                (home, t),
                ex_send.at[dy * 2 + t],
                ex_recv.at[cross],
                own,
            )
    keeper = core + cross * (1 - 2 * core)

    def query_copy(dy):
        yy = (y + dy) % 4
        cols = pl.ds(pl.multiple_of(yy * GROUP, GROUP), GROUP)
        return pltpu.make_async_remote_copy(
            src_ref=q_ref.at[:, cols],
            dst_ref=qr_ref.at[y],
            send_sem=q_send.at[dy],
            recv_sem=q_recv,
            device_id=(chip(x, zt, yy), keeper),
            device_id_type=MESH,
        )

    def send_queries():
        @pl.when(cross == 0)
        def _():
            cols = pl.ds(pl.multiple_of(y * GROUP, GROUP), GROUP)
            pltpu.make_async_copy(q_ref.at[:, cols], qr_ref.at[y], q_recv).start()

        @pl.when(cross != 0)
        def _():
            query_copy(0).start()

        for dy in range(1, 4):
            query_copy(dy).start()

    def part(t, xs, zs):
        return kv_ref.at[t, pl.ds(xs * 16 + zs * 4, 4)]

    def arrive(t, xs, zs, sem):
        ref = part(t, xs, zs)
        pltpu.make_async_copy(ref, ref, sem).wait()

    def run(t, steps):
        sends = []
        for turn, (kind, xs, zs, targets) in enumerate(steps):
            if turn == 2:
                send_queries()
            if kind == "own":
                arrive(t, xs, zs, ex_recv.at[0])
            elif kind == "pair":
                arrive(t, xs, zs, ex_recv.at[1])
            else:
                arrive(t, xs, zs, ag_recv.at[xs * 4 + zs])
            for device in targets:
                copy = pltpu.make_async_remote_copy(
                    src_ref=part(t, xs, zs),
                    dst_ref=part(t, xs, zs),
                    send_sem=ag_send.at[len(sends)],
                    recv_sem=ag_recv.at[xs * 4 + zs],
                    device_id=device,
                    device_id_type=MESH,
                )
                copy.start()
                sends.append(copy)
            copy = pltpu.make_async_remote_copy(
                src_ref=part(t, xs, zs),
                dst_ref=part(t, xs, zs),
                send_sem=dd_send.at[xs * 4 + zs],
                recv_sem=dd_recv.at[xs * 4 + zs],
                device_id=twin,
                device_id_type=MESH,
            )
            copy.start()
        for copy in sends:
            copy.wait_send()

    @pl.when(core == 0)
    def _():
        run(
            0,
            (
                ("own", x, z, (across, right, left)),
                ("pair", x, zo, (across, left, right)),
                ("got", x, za, (right, left)),
                ("got", x, zao, (left, right)),
                ("got", xl, z, (right,)),
                ("got", xr, z, ()),
                ("got", xr, zo, (left,)),
                ("got", xl, zo, ()),
                ("got", xl, za, (right,)),
                ("got", xr, za, ()),
                ("got", xr, zao, (left,)),
                ("got", xl, zao, ()),
                ("got", xo, z, ()),
                ("got", xo, zo, ()),
                ("got", xo, za, ()),
                ("got", xo, zao, ()),
            ),
        )

    @pl.when(core == 1)
    def _():
        run(
            1,
            (
                ("own", x, z, (right, left, across)),
                ("pair", x, zo, (left, right, across)),
                ("got", xl, z, (right, across)),
                ("got", xr, z, (across,)),
                ("got", xr, zo, (left, across)),
                ("got", xl, zo, (across,)),
                ("got", x, za, ()),
                ("got", x, zao, ()),
                ("got", xo, z, (across,)),
                ("got", xo, zo, (across,)),
                ("got", xl, za, ()),
                ("got", xr, za, ()),
                ("got", xr, zao, ()),
                ("got", xl, zao, ()),
                ("got", xo, za, ()),
                ("got", xo, zao, ()),
            ),
        )

    for piece in range(16):
        ref = kv_ref.at[1 - core, pl.ds(piece * 4, 4)]
        pltpu.make_async_copy(ref, ref, dd_recv.at[piece]).wait()
        ref = kv_ref.at[core, pl.ds(piece * 4, 4)]
        pltpu.make_async_copy(ref, ref, dd_send.at[piece]).wait()
    pltpu.make_async_copy(qr_ref, qr_ref, q_recv).wait()

    @pl.when(cross != 0)
    def _():
        query_copy(0).wait_send()

    for dy in range(1, 4):
        query_copy(dy).wait_send()

    for own, copy in finish:
        if own is None:
            copy.wait_send()
        else:

            @pl.when(jnp.logical_not(own))
            def _():
                copy.wait_send()


def spread(queries, keys, values):
    return pl.pallas_call(
        spread_kernel,
        out_shape=(
            jax.ShapeDtypeStruct((4, ROWS, GROUP), jnp.bfloat16),
            jax.ShapeDtypeStruct((2, SLOTS, ROWS, HEAD), jnp.bfloat16),
        ),
        in_specs=[pl.BlockSpec(memory_space=pltpu.HBM)] * 3,
        out_specs=[pl.BlockSpec(memory_space=pltpu.VMEM)] * 2,
        scratch_shapes=[
            pltpu.SemaphoreType.DMA((8,)),
            pltpu.SemaphoreType.DMA((2,)),
            pltpu.SemaphoreType.DMA((4,)),
            pltpu.SemaphoreType.DMA,
            pltpu.SemaphoreType.DMA((14,)),
            pltpu.SemaphoreType.DMA((16,)),
            pltpu.SemaphoreType.DMA((16,)),
            pltpu.SemaphoreType.DMA((16,)),
        ],
        compiler_params=pltpu.CompilerParams(
            collective_id=0, has_side_effects=True, vmem_limit_bytes=8 * 1024 * 1024
        ),
        cost_estimate=pl.CostEstimate(flops=20_000_000_000, bytes_accessed=40_000_000, transcendentals=0),
        name="spread",
    )(queries, keys, values)


WIDTH = 4 * SPAN
ITEMS = 96
UNROLL = 8
HUGE = 2.0**100
FACTOR = HEAD ** (-0.5) * 1.4426950408889634


def attend_kernel(
    span_ref, doc_ref, q_ref, kv_ref, o_ref, slot_ref, item_q, item_low, item_first, qa_ref, s_ref, p_ref, acc_ref
):
    cp, core, x, z, y, band, cross = place()
    zs = z + cross * (3 - 2 * z)

    def invert(slot, carry):
        slot_ref[span_ref[slot]] = slot
        return carry

    lax.fori_loop(0, 2 * SLOTS, invert, 0, unroll=True)
    docs = doc_ref[...]
    starts = [jnp.int32(0)]
    counts = [jnp.sum((docs < d).astype(jnp.float32), axis=0, keepdims=True) for d in range(1, 8)]
    counts = jnp.sum(jnp.concatenate(counts + [counts[0]], axis=0), axis=1, keepdims=True).astype(jnp.int32)
    starts += [counts[d, 0] for d in range(7)]
    ends = starts[1:] + [jnp.int32(KEYS)]
    lane = lax.broadcasted_iota(jnp.int32, (1, HEAD), 1)
    start = jnp.where(lane == 104, -KEYS, KEYS)
    end = jnp.zeros((1, HEAD), jnp.int32)
    for d in range(8):
        start = jnp.where(lane == d, starts[d], start)
        end = jnp.where(lane == d, ends[d], end)

    def record(at, index, low, first):
        item_q[at] = index
        item_low[at] = low
        item_first[at] = first

    row = lax.broadcasted_iota(jnp.int32, (SPAN, HEAD), 0)
    col = lax.broadcasted_iota(jnp.int32, (SPAN, HEAD), 1)
    later = ((col >= 8) & (col < 104) & (col - 8 > row)) | (col == 104)
    later = jnp.where(later, -HUGE, 0.0)
    reach = jnp.where(lane < 8, start, -KEYS)
    limit = jnp.where(lane < 8, end, 2 * KEYS)
    heads = [(begin, begin // SPAN) for begin in starts]

    def plan(index, at):
        span = span_ref[2 * chip(x, zs, index // 2) + index % 2]
        first = span * SPAN
        same = (row >= reach - first) & (row < limit - first)
        qa_ref[index] = jnp.where(same, later, -HUGE).astype(jnp.bfloat16)
        acc_ref[index] = jnp.zeros((HEAD + 16, WIDTH), jnp.float32)
        lowest = jnp.int32(0)
        for begin, head in heads[1:]:
            lowest = jnp.where(first >= begin, head, lowest)
        for turn in range(9):
            record(at + turn, index, span - 3 - 4 * turn, 1 if turn == 0 else 0)
        return at + ((span - lowest + 4) >> 2)

    for at in range(2):
        record(at, 8, 0, 0)
    total = lax.fori_loop(0, 8, plan, jnp.int32(2), unroll=2)
    for at in range(UNROLL + 2):
        record(total + at, 8, 0, 0)
    s_ref[1] = jnp.zeros((BLOCK, WIDTH), jnp.float32)
    p_ref[0] = jnp.zeros((BLOCK, WIDTH), jnp.bfloat16)
    acc_ref[8] = jnp.zeros((HEAD + 16, WIDTH), jnp.float32)
    qa_ref[8] = jnp.zeros((SPAN, HEAD), jnp.bfloat16)
    row = lax.broadcasted_iota(jnp.int32, (BLOCK, HEAD), 0)
    col = lax.broadcasted_iota(jnp.int32, (BLOCK, HEAD), 1)
    corner = jnp.where(row >= BLOCK - SPAN, row - (BLOCK - SPAN) + 8, -1)

    def fetch(which, low):
        slots = [slot_ref[jnp.maximum(low + j, 0)] for j in range(4)]
        return jnp.concatenate([kv_ref[which, slot] for slot in slots], axis=0)

    def step(at, parity, state):
        best, fade = state
        low = item_low[at + 2]
        base = low * SPAN
        seen = (row >= start - base) & (row < end - base)
        seen = seen | (corner + (1 - item_first[at + 2]) * 4096 == col)
        extra = jnp.where(seen, 1.0, 0.0).astype(jnp.bfloat16)
        keys = jnp.concatenate([fetch(0, low), extra], axis=1)
        index = item_q[at + 2]
        source = jnp.minimum(index, 7)
        rows = pl.ds(pl.multiple_of((source % 2) * SPAN, SPAN), SPAN)
        q = q_ref[source // 2, rows, :]
        q = jnp.concatenate([q[:, h * HEAD : (h + 1) * HEAD] for h in range(4)], axis=0)
        q = jnp.concatenate([q, jnp.concatenate([qa_ref[index]] * 4, axis=0)], axis=1)
        s_ref[parity] = lax.dot_general(keys, q, (((1,), (1,)), ((), ())), preferred_element_type=jnp.float32)

        s = s_ref[1 - parity]
        best = jnp.where(item_first[at + 1] == 1, NEG, best)
        new = jnp.maximum(best, jnp.max(s, axis=0, keepdims=True))
        p_ref[1 - parity] = jnp.exp2(s * FACTOR - new * FACTOR).astype(jnp.bfloat16)

        v = fetch(1, item_low[at])
        v = jnp.concatenate([v.T, jnp.ones((16, BLOCK), jnp.bfloat16)], axis=0)
        index = item_q[at]
        acc_ref[index] = acc_ref[index] * fade + jnp.dot(v, p_ref[parity], preferred_element_type=jnp.float32)
        return new, jnp.exp2((best - new) * FACTOR)

    def several(turn, state):
        for k in range(UNROLL):
            state = step(UNROLL * turn + k, k % 2, state)
        return state

    turns = total // UNROLL
    state = (jnp.full((1, WIDTH), NEG, jnp.float32), jnp.zeros((1, WIDTH), jnp.float32))
    state = lax.fori_loop(0, turns, several, state)

    def couple(turn, state):
        for k in range(2):
            state = step(UNROLL * turns + 2 * turn + k, k, state)
        return state

    lax.fori_loop(0, (total - UNROLL * turns + 1) >> 1, couple, state)

    def finish(index, carry):
        rows = pl.ds(pl.multiple_of((index % 2) * SPAN, SPAN), SPAN)
        out = (acc_ref[index, 0:HEAD] * (1.0 / acc_ref[index, HEAD : HEAD + 1])).T.astype(jnp.bfloat16)
        for h in range(4):
            o_ref[index // 2, rows, h * HEAD : (h + 1) * HEAD] = out[h * SPAN : (h + 1) * SPAN]
        return carry

    lax.fori_loop(0, 8, finish, 0, unroll=4)


def attend(span_table, doc_ids, q, kv):
    return pl.pallas_call(
        attend_kernel,
        out_shape=jax.ShapeDtypeStruct((4, ROWS, GROUP), jnp.bfloat16),
        in_specs=[
            pl.BlockSpec(memory_space=pltpu.SMEM),
            pl.BlockSpec(memory_space=pltpu.VMEM),
            pl.BlockSpec(memory_space=pltpu.VMEM),
            pl.BlockSpec(memory_space=pltpu.VMEM),
        ],
        out_specs=pl.BlockSpec(memory_space=pltpu.VMEM),
        scratch_shapes=[
            pltpu.SMEM((2 * SLOTS,), jnp.int32),
            pltpu.SMEM((ITEMS,), jnp.int32),
            pltpu.SMEM((ITEMS,), jnp.int32),
            pltpu.SMEM((ITEMS,), jnp.int32),
            pltpu.VMEM((9, SPAN, HEAD), jnp.bfloat16),
            pltpu.VMEM((2, BLOCK, WIDTH), jnp.float32),
            pltpu.VMEM((2, BLOCK, WIDTH), jnp.bfloat16),
            pltpu.VMEM((9, HEAD + 16, WIDTH), jnp.float32),
        ],
        compiler_params=pltpu.CompilerParams(vmem_limit_bytes=24 * 1024 * 1024),
        name="attend",
    )(span_table, doc_ids.reshape(KEYS // 128, 128), q, kv.reshape(2, 2 * SLOTS, SPAN, HEAD))


CHUNK = 512
CHUNKS = 8


def project_kernel(
    o_ref, w_ref, out_ref, attn, weight, partial, share, theirs, w_sem, b_send, b_recv, s_send, s_recv
):
    cp, core, x, z, y, band, cross = place()
    for n in range(CHUNKS):
        pltpu.make_async_copy(w_ref.at[:, pl.ds(n * CHUNK, CHUNK)], weight.at[n], w_sem.at[n]).start()
    zs = z + cross * (3 - 2 * z)
    barrier = pltpu.get_barrier_semaphore()
    pl.semaphore_signal(barrier, inc=1, device_id=(cp, 1 - core), device_id_type=MESH)
    for dy in range(1, 4):
        pl.semaphore_signal(barrier, inc=1, device_id=(chip(x, zs, (y + dy) % 4), band), device_id_type=MESH)

    @pl.when(cross != 0)
    def _():
        pl.semaphore_signal(barrier, inc=1, device_id=(chip(x, zs, y), band), device_id_type=MESH)

    pl.semaphore_wait(barrier, 4 + cross)
    copies = []
    for dy in (0, 1, 3, 2):
        yy = (y + dy) % 4
        src, dst = o_ref.at[yy], attn.at[y]
        copy = pltpu.make_async_remote_copy(
            src_ref=src,
            dst_ref=dst,
            send_sem=b_send.at[dy],
            recv_sem=b_recv.at[y],
            device_id=(chip(x, zs, yy), band),
            device_id_type=MESH,
        )
        copies.append(copy)
        if dy == 0:

            @pl.when(cross == 0)
            def _():
                pltpu.make_async_copy(src, dst, b_recv.at[y]).start()

            @pl.when(cross != 0)
            def _():
                copy.start()
        else:
            copy.start()
    mine = pl.ds(pl.multiple_of(core * SPAN, SPAN), SPAN)
    yours = pl.ds(pl.multiple_of((1 - core) * SPAN, SPAN), SPAN)

    def give(n):
        return pltpu.make_async_remote_copy(
            src_ref=share.at[n, yours],
            dst_ref=theirs.at[n],
            send_sem=s_send.at[n],
            recv_sem=s_recv.at[n],
            device_id=(cp, 1 - core),
            device_id_type=MESH,
        )

    def gain(k, n):
        rows = pl.ds(pl.multiple_of(k * GROUP, GROUP), GROUP)
        return jnp.dot(attn[k], weight[n, rows, :], preferred_element_type=jnp.float32)

    for n in range(CHUNKS):
        pltpu.make_async_copy(weight.at[n], weight.at[n], w_sem.at[n]).wait()
    def block(dy):
        return (y + dy) % 4

    def await_block(dy):
        pltpu.make_async_copy(attn.at[block(dy)], attn.at[block(dy)], b_recv.at[block(dy)]).wait()

    for dy in (0, 3, 1):
        await_block(dy)
    for n in range(CHUNKS):
        partial[n] = gain(block(0), n) + gain(block(3), n) + gain(block(1), n)
    await_block(2)
    for n in range(CHUNKS):
        share[n] = (partial[n] + gain(block(2), n)).astype(jnp.bfloat16)
        give(n).start()

    def add(n, carry):
        give(n).wait()
        cols = pl.ds(pl.multiple_of(n * CHUNK, CHUNK), CHUNK)
        total = share[n, mine, :].astype(jnp.float32) + theirs[n].astype(jnp.float32)
        out_ref[:, cols] = total.astype(jnp.bfloat16)
        return carry

    lax.fori_loop(0, CHUNKS, add, 0)
    for turn, copy in enumerate(copies):
        if turn == 0:

            @pl.when(cross != 0)
            def _():
                copy.wait_send()
        else:
            copy.wait_send()


def project(o, weight):
    return pl.pallas_call(
        project_kernel,
        out_shape=jax.ShapeDtypeStruct((SPAN, 4096), jnp.bfloat16),
        in_specs=[pl.BlockSpec(memory_space=pl.ANY), pl.BlockSpec(memory_space=pltpu.HBM)],
        out_specs=pl.BlockSpec(memory_space=pltpu.VMEM),
        scratch_shapes=[
            pltpu.VMEM((4, ROWS, GROUP), jnp.bfloat16),
            pltpu.VMEM((CHUNKS, 2048, CHUNK), jnp.bfloat16),
            pltpu.VMEM((CHUNKS, ROWS, CHUNK), jnp.float32),
            pltpu.VMEM((CHUNKS, ROWS, CHUNK), jnp.bfloat16),
            pltpu.VMEM((CHUNKS, SPAN, CHUNK), jnp.bfloat16),
            pltpu.SemaphoreType.DMA((CHUNKS,)),
            pltpu.SemaphoreType.DMA((4,)),
            pltpu.SemaphoreType.DMA((4,)),
            pltpu.SemaphoreType.DMA((CHUNKS,)),
            pltpu.SemaphoreType.DMA((CHUNKS,)),
        ],
        compiler_params=pltpu.CompilerParams(
            collective_id=1, has_side_effects=True, vmem_limit_bytes=32 * 1024 * 1024
        ),
        name="project",
    )(o, weight)


def local(queries, keys, values, span_table, doc_ids, out_weight):
    far = lambda value: pltpu.with_memory_space_constraint(value, pltpu.HBM)
    q, kv = spread(far(queries), far(keys), far(values))
    o = attend(span_table, doc_ids, q, kv)
    return project(o, far(out_weight))


def solution(mesh):
    return jax.shard_map(
        local,
        mesh=mesh,
        in_specs=(P("cp", "hd"), P("cp", "hd"), P("cp", "hd"), P(), P(), P("hd", None)),
        out_specs=P(("cp", "hd"), None),
        check_vma=False,
    )
```
